32 devices in a mesh: section: 2 (over core), node: 4 (over z), local: 4 (over y, x).
Axes of the slice: x: 2, y: 2, z: 4, core: 2. Of those that a mesh axis runs over, the one named last changes fastest.
Arguments:
- tokens: bfloat16 [2, 1024, 768], P(None, ('node', 'local')), may hold values from -18 to 18
- expert_ids: int32 [2, 2, 1024, 2], P('section', None, ('node', 'local')), may hold values from 0 to 15, as said below
- slots: int32 [2, 2, 1024, 2], P('section', None, ('node', 'local')), may hold values from -1 to 31, as said below
- gates: float32 [2, 2, 1024, 2], P('section', None, ('node', 'local')), may hold values from 0.2 to 1
- gain: float32 [2, 768], P('section'), may hold values from 0.5 to 1.5
- w_gate: bfloat16 [2, 16, 768, 3072], P('section', ('node', 'local')), may hold values from -0.21875 to 0.21875
- w_up: bfloat16 [2, 16, 768, 3072], P('section', ('node', 'local')), may hold values from -0.21875 to 0.21875
- w_down: bfloat16 [2, 16, 3072, 768], P('section', ('node', 'local')), may hold values from -0.109375 to 0.109375
Outputs:
- hidden: bfloat16 [2, 2, 1024, 768], P('section', None, ('node', 'local'))
The draws below stay inside these ranges and needn't reach their ends.
Inputs may be any that keep to these rules, and one draw needn't show every extreme that they name: `expert_ids`: in each layer and micro-batch the two ids of a token differ, no expert is named by more than 256 tokens, and some expert is named by exactly 256. Expert e lies on node e // 4. Among one device's 64 tokens of a micro-batch and layer, the kept tokens that reach one node hold distinct slots below 32, and the two choices of a token on one node carry the same slot; -1 marks a dropped choice.
All inputs are finite; a program needn't handle non-finite values.
Results may differ from the reference program's by a relative error of at most 0.0085.
Values may be sent and summed in bfloat16 or wider, within the bound.
A program may use at most 64 MiB of HBM per device.

```python
import math
import jax
import jax.numpy as jnp
from jax import lax

D = 768
FF = 3072
TOP = 2
TOK_MB = 64
MICRO = 2
LAYERS = 2
EXPERTS = 16
TOKENS = 1024
CAP = 32
ECAP = 256
N_NODE = 4
N_LOCAL = 4


def one_group(group_key):
    subkeys = jax.random.split(group_key, 5)
    node_order = jax.random.permutation(subkeys[0], N_NODE)
    local_order = jax.random.permutation(subkeys[1], N_LOCAL)
    second_node_order = jax.random.permutation(subkeys[4], N_NODE)
    half_count = EXPERTS // 2
    quarter = EXPERTS // 4
    half_local = N_LOCAL // 2
    mean_load = 2 * TOK_MB
    rank_ids = jnp.arange(half_count, dtype=jnp.int32)
    upper_gain = mean_load * (quarter - rank_ids) // quarter
    lower_gain = mean_load * (quarter - (half_count - 1 - rank_ids)) // quarter
    quotas = jnp.where(rank_ids < quarter, mean_load + upper_gain, mean_load - lower_gain)
    bounds = jnp.cumsum(quotas)
    places = jnp.arange(TOKENS, dtype=jnp.int32)
    which_rank = jnp.sum((places[:, None] >= bounds[None, :]).astype(jnp.int32), axis=1)
    first_node = node_order[which_rank // half_local]
    second_node = second_node_order[which_rank // half_local]
    first_ids = first_node * N_LOCAL + local_order[which_rank % half_local]
    second = second_node * N_LOCAL + local_order[half_local + which_rank % half_local]
    first_ids = first_ids[jax.random.permutation(subkeys[2], TOKENS)]
    second = second[jax.random.permutation(subkeys[3], TOKENS)]
    routing = jnp.stack([first_ids, second], axis=1).astype(jnp.int32)
    device_route = routing.reshape(N_NODE * N_LOCAL, TOK_MB, 2)
    node_route = device_route // N_LOCAL
    node_span = jnp.arange(N_NODE, dtype=jnp.int32)
    touched = ((node_route[..., 0:1] == node_span) | (node_route[..., 1:2] == node_span)).astype(jnp.int32)
    before = jnp.cumsum(touched, axis=1) - touched
    slot_pick = jnp.take_along_axis(before, node_route, axis=2)
    slot_vals = jnp.where(slot_pick < CAP, slot_pick, -1).reshape(TOKENS, 2).astype(jnp.int32)
    return (routing, slot_vals)


def route_tables(key):
    base_key = jax.random.fold_in(key, 7)
    group_keys = jax.random.split(base_key, LAYERS * MICRO)
    expert_table, slot_table = jax.vmap(one_group)(group_keys)
    return (expert_table.reshape(LAYERS, MICRO, TOKENS, 2), slot_table.reshape(LAYERS, MICRO, TOKENS, 2))


def draw_expert_ids(key, part):
    return route_tables(key)[0]


def draw_slots(key, part):
    return route_tables(key)[1]


def draw_tokens(key, part):
    subkeys = jax.random.split(jax.random.fold_in(key, 3), 2)
    values = jnp.clip(jax.random.normal(subkeys[0], (MICRO, TOKENS, D), jnp.float32), -6.0, 6.0)
    scales = jnp.exp(jax.random.uniform(subkeys[1], (MICRO, TOKENS, 1), jnp.float32, math.log(0.5), math.log(2.0)))
    return (values * scales).astype(jnp.bfloat16)


def steps_of(key, shape, cuts, low, high):
    level = 1.0
    for dim, shards_of in cuts:
        draws = jax.random.uniform(jax.random.fold_in(jax.random.fold_in(key, 6), dim), (shards_of,), jnp.float32, low / len(cuts), high / len(cuts))
        level = level * jnp.repeat(jnp.exp(draws), shape[dim] // shards_of).reshape((-1,) + (1,) * (len(shape) - 1 - dim))
    return level


def centred(own_key, dims, deviation, most, pieces=(), kind=jnp.bfloat16):
    result = jax.random.normal(own_key, dims, jnp.float32) * deviation
    if len(pieces) > 0:
        result = steps_of(own_key, dims, pieces, -0.22, 0.18) * result
    return jnp.clip(result, min=-most, max=most).astype(kind)


def setup_inputs(seed: int = 0) -> dict:
    key_list = jax.random.split(jax.random.key(seed), 9)
    tokens = draw_tokens(jax.random.fold_in(key_list[8], 71), 0)
    expert_ids = draw_expert_ids(jax.random.fold_in(key_list[8], 71), 0)
    slots = draw_slots(jax.random.fold_in(key_list[8], 71), 0)
    gates = jnp.clip(0.2 + 0.8 * jax.random.uniform(key_list[3], (LAYERS, MICRO, TOKENS, TOP), jnp.float32) ** steps_of(key_list[3], (LAYERS, MICRO, TOKENS, TOP), ((0, 2), (2, 16)), -0.2, 0.2), 0.2, 1.0)
    gain = jnp.clip(1.0 + 0.1 * jax.random.normal(key_list[4], (LAYERS, D), jnp.float32), 0.5, 1.5)
    w_gate = centred(key_list[5], (LAYERS, EXPERTS, D, FF), D ** -0.5, 0.21875, ((0, 2), (1, 16)))
    w_up = centred(key_list[6], (LAYERS, EXPERTS, D, FF), D ** -0.5, 0.21875, ((0, 2), (1, 16)))
    w_down = centred(key_list[7], (LAYERS, EXPERTS, FF, D), FF ** -0.5, 0.109375, ((0, 2), (1, 16)))
    return {"tokens": tokens, "expert_ids": expert_ids, "slots": slots, "gates": gates, "gain": gain, "w_gate": w_gate, "w_up": w_up, "w_down": w_down}


def rms_normed(values, gain_row):
    floats = values.astype(jnp.float32)
    mean_square = lax.optimization_barrier(jnp.mean(floats * floats, axis=-1, keepdims=True))
    return (floats * lax.rsqrt(mean_square + 1e-05) * gain_row).astype(jnp.bfloat16)

def expert_apply(picked, gate_mat, up_mat, down_mat):
    gate_act = jnp.dot(picked, gate_mat, preferred_element_type=jnp.float32)
    up_act = jnp.dot(picked, up_mat, preferred_element_type=jnp.float32)
    inner = (jax.nn.gelu(gate_act, approximate=True) * up_act).astype(jnp.bfloat16)
    return jnp.dot(inner, down_mat, preferred_element_type=jnp.float32)

def moe_layer(layer_in, routing, slot_ids, gate_vals, gain_row, gate_all, up_all, down_all):
    normed = rms_normed(layer_in, gain_row)
    keep_weight = jnp.where(slot_ids >= 0, gate_vals, jnp.float32(0.0)).astype(jnp.float32)

    def per_expert(totals, expert):
        hit_mask = routing == expert
        any_hit = jnp.any(hit_mask, axis=1)
        row_index = jnp.nonzero(any_hit, size=ECAP, fill_value=0)[0].astype(jnp.int32)
        valid_rows = jnp.arange(ECAP, dtype=jnp.int32) < jnp.sum(any_hit.astype(jnp.int32))
        picked = normed[row_index]
        outputs = expert_apply(picked, gate_all[expert], up_all[expert], down_all[expert])
        row_weight = lax.optimization_barrier(jnp.sum(jnp.where(hit_mask, keep_weight, jnp.float32(0.0)), axis=1))[row_index]
        row_weight = jnp.where(valid_rows, row_weight, jnp.float32(0.0))
        scaled = lax.optimization_barrier((row_weight[:, None] * outputs).astype(jnp.bfloat16)).astype(jnp.float32)
        choice_mask = (hit_mask[row_index] & valid_rows[:, None]).astype(jnp.float32)
        totals = totals.at[row_index].add(scaled[:, None, :] * choice_mask[:, :, None])
        return (totals, None)
    start = jnp.zeros((layer_in.shape[0], 2, layer_in.shape[1]), jnp.float32)
    totals, _ = lax.scan(per_expert, start, jnp.arange(EXPERTS, dtype=jnp.int32))
    same_node = routing[:, 0] // N_LOCAL == routing[:, 1] // N_LOCAL
    pair_sum = totals[:, 0] + totals[:, 1]
    together = lax.optimization_barrier(pair_sum.astype(jnp.bfloat16)).astype(jnp.float32)
    mixed_rows = jnp.where(same_node[:, None], together, pair_sum)
    return (layer_in.astype(jnp.float32) + mixed_rows).astype(jnp.bfloat16)

def reference(tokens, expert_ids, slots, gates, gain, w_gate, w_up, w_down):
    current = [tokens[batch_index] for batch_index in range(MICRO)]
    stacked = []
    for layer_index in range(LAYERS):
        produced = []
        for batch_index in range(MICRO):
            produced.append(moe_layer(current[batch_index], expert_ids[layer_index, batch_index], slots[layer_index, batch_index], gates[layer_index, batch_index], gain[layer_index], w_gate[layer_index], w_up[layer_index], w_down[layer_index]))
        stacked.append(jnp.stack(produced))
        current = produced
    return jnp.stack(stacked)
```

```python
import functools

import jax
import jax.numpy as jnp
from jax import lax
from jax.experimental import pallas as pl
from jax.experimental.pallas import tpu as pltpu
from jax.sharding import PartitionSpec as P

MESH = pl.DeviceIdType.MESH
LANES = 128
NS = jax.named_scope


def relay_kernel(
    sizes,
    tok_hbm, ids_hbm, slots_hbm, gates_hbm, gain_hbm, wg_hbm, wu_hbm, wd_hbm,
    out_ref,
    tok, ids, slots, gates, gain, held, packed, relay, arrived, answer, parts, summed, back,
    hits, hits_t, first_t, meta_out, meta_z, meta_in, pick, pick_t, pick_w,
    xs, inner, scaled, wg, wu, wd,
    in_sem, w_sem, first_send, first_recv, mz_send, mz_recv, mo_send, mo_recv, mf_send, mf_recv,
    z_send, z_recv, own_send, own_recv, fan_send, fan_recv, part_send, part_recv,
    back_send, back_recv, relay_send, relay_recv,
):
    n_node, n_local, micro, toks, width, cap, limit, chunks, ff_chunks = sizes
    n = n_node * n_local
    total = n * cap
    cw = width // chunks
    fw = inner.shape[1] // ff_chunks
    half = jnp.bfloat16
    sec = lax.axis_index("section")
    node = lax.axis_index("node")
    local = lax.axis_index("local")
    me = local * n_node + node

    def near(k):
        if n_node != 4:
            return lax.rem(node + k, n_node)
        j = jnp.int32(0)
        for z in range(n_node):
            order = sorted((p for p in range(n_node) if p != z), key=lambda p: abs(p - z))
            j = jnp.where(node == z, order[k - 1], j)
        return j

    others = [near(k) for k in range(1, n_node)]
    plane = [lax.rem(local + i, n_local) for i in range(1, n_local)]

    def remote(src, dst, send, recv, **to):
        return pltpu.make_async_remote_copy(
            src, dst, send, recv, device_id=to, device_id_type=MESH
        )

    def got(ref, sem):
        remote(ref, ref, sem, sem, section=1 - sec).wait_recv()

    def sent(ref, sem):
        remote(ref, ref, sem, sem, section=1 - sec).wait_send()

    barrier = pltpu.get_barrier_semaphore()

    def greet(**to):
        pl.semaphore_signal(barrier, inc=1, device_id=to, device_id_type=MESH)

    greet(section=1 - sec)
    for j in others:
        greet(section=1 - sec, node=j)
    for i in plane:
        greet(local=i)
        greet(section=1 - sec, local=i)

    @pl.when(sec == 1)
    def _():
        for j in others:
            greet(node=j)

    loads = [
        pltpu.make_async_copy(src, dst, in_sem.at[i])
        for i, (src, dst) in enumerate(
            ((ids_hbm, ids), (slots_hbm, slots), (gates_hbm, gates), (tok_hbm, tok), (gain_hbm, gain))
        )
    ]
    for load in loads:
        load.start()
    weights_in = [
        pltpu.make_async_copy(src, dst, w_sem.at[i])
        for i, (src, dst) in enumerate(((wg_hbm, wg), (wu_hbm, wu), (wd_hbm, wd)))
    ]
    for load in loads:
        load.wait()
    for copy in weights_in:
        copy.start()

    slot_span = lax.broadcasted_iota(jnp.int32, (n_node * cap, toks), 0)
    for mb in range(micro):
        hit = None
        for k in range(2):
            e = ids[mb, k : k + 1, :]
            s = slots[mb, k : k + 1, :]
            pos = jnp.where(s >= 0, lax.div(e, jnp.full_like(e, n_local)) * cap + s, -1)
            this = jnp.where(pos == slot_span, 1.0, 0.0)
            hit = this if hit is None else jnp.maximum(hit, this)
        hits[mb] = hit.astype(half)
        hits_t[mb] = hit.T.astype(half)

    def note_weights():
        exp_span = lax.broadcasted_iota(jnp.int32, (n, toks), 0)
        lane_span = lax.broadcasted_iota(jnp.int32, (LANES, toks), 0)
        my_lane = lax.rem(me * cap, LANES)
        for mb in range(micro):
            named = []
            lanes = []
            for k in range(2):
                e = ids[mb, k : k + 1, :]
                s = slots[mb, k : k + 1, :]
                lane = jnp.where(s >= 0, my_lane + s, -1)
                named.append(jnp.where(e == exp_span, gates[mb, k : k + 1, :], 0.0))
                lanes.append(jnp.where(lane == lane_span, 1.0, 0.0))
            weights = lax.dot_general(
                jnp.concatenate(named, axis=1),
                jnp.concatenate(lanes, axis=1),
                (((1,), (1,)), ((), ())),
                precision=lax.Precision.HIGHEST,
                preferred_element_type=jnp.float32,
            )
            for j in range(n_node):
                meta_out[j, mb * n_local : (mb + 1) * n_local] = weights[
                    j * n_local : (j + 1) * n_local
                ]
        meta_in[me] = meta_out[node]

    def pack(mb, h):
        floats = h.astype(jnp.float32)
        mean_square = jnp.mean(floats * floats, axis=-1, keepdims=True)
        normed = (floats * lax.rsqrt(mean_square + 1e-05) * gain[...]).astype(half)
        rows = jnp.dot(hits[mb], normed, preferred_element_type=jnp.float32)
        for j in range(n_node):
            packed[mb, j] = rows[j * cap : (j + 1) * cap].astype(half)
        arrived[mb, local, node] = packed[mb, node]

    def own_fan(mb, recv):
        for i in plane:
            remote(
                packed.at[mb, node], arrived.at[mb, local, node], own_send.at[mb], recv, local=i
            ).start()

    def flat(blocks):
        if cap % 16:
            blocks = blocks.astype(jnp.float32)
        return blocks.reshape(-1, blocks.shape[-1]).astype(half)

    def places():
        upto = lax.broadcasted_iota(jnp.int32, (total, total), 0) <= lax.broadcasted_iota(
            jnp.int32, (total, total), 1
        )
        upto = jnp.where(upto, 1.0, 0.0).astype(half)
        spot = lax.broadcasted_iota(jnp.int32, (limit, total), 0).astype(jnp.float32)
        per_group = LANES // cap
        for mb in range(micro):
            mine = pl.ds(mb * n_local + local, 1)
            w_row = jnp.concatenate(
                [
                    sum(meta_in[g * per_group + b, mine, :] for b in range(per_group))
                    for g in range(total // LANES)
                ],
                axis=1,
            )
            w_rows = jnp.broadcast_to(w_row, (8, total))
            chosen = jnp.where(w_rows > 0.0, 1.0, 0.0)
            rank = jnp.dot(chosen.astype(half), upto, preferred_element_type=jnp.float32)
            rank = jnp.where(w_rows > 0.0, rank - 1.0, -1.0)
            is_at = spot == jnp.broadcast_to(rank[0:1], (limit, total))
            place = jnp.where(is_at, 1.0, 0.0)
            pick[mb] = place.astype(half)
            pick_t[mb] = place.T.astype(half)
            pick_w[mb] = jnp.sum(
                jnp.where(is_at, jnp.broadcast_to(w_row, (limit, total)), 0.0),
                axis=1, keepdims=True,
            )

    def hand_second(mb):
        for j in others:
            block = arrived.at[mb, local, j]
            got(block, z_recv.at[1, mb, j])
            for i in plane:
                remote(block, block, fan_send.at[1, mb], fan_recv.at[mb], local=i).start()

    def expert(mb, carry):
        @pl.when(sec == 0)
        def _():
            with NS("fan"):
                got(arrived.at[mb, pl.ds(0, n_local - 1), 0], own_recv.at[mb])
                got(arrived.at[mb, :, pl.ds(0, n_node - 1)], fan_recv.at[mb])

        @pl.when(sec == 1)
        def _():
            with NS("fan"):
                got(arrived.at[mb, pl.ds(0, n_local - 1)], fan_recv.at[mb])

        with NS("pick"):
            xs[...] = jnp.dot(
                pick[mb], flat(arrived[mb]), preferred_element_type=jnp.float32
            ).astype(half)

        @pl.when(mb == 0)
        def _():
            for copy in weights_in:
                copy.wait()

        with NS("up"):
            for f in range(ff_chunks):
                cols = slice(f * fw, (f + 1) * fw)
                x = xs[...]
                gate = jnp.dot(x, wg[:, cols], preferred_element_type=jnp.float32)
                up = jnp.dot(x, wu[:, cols], preferred_element_type=jnp.float32)
                inner[:, cols] = (jax.nn.gelu(gate, approximate=True) * up).astype(half)
                if f == ff_chunks // 3 - 1:

                    @pl.when(jnp.logical_and(sec == 1, mb + 1 < micro))
                    def _():
                        hand_second(mb + 1)

        def down(c):
            acc = jnp.dot(
                inner[...], wd[:, c * cw : (c + 1) * cw], preferred_element_type=jnp.float32
            )
            scaled[c] = (pick_w[mb] * acc).astype(half)

        with NS("down"):
            down(0)
            for c in range(chunks):
                if c + 1 < chunks:
                    down(c + 1)
                spread = jnp.dot(pick_t[mb], scaled[c], preferred_element_type=jnp.float32)
                answer[mb, c] = spread.reshape(n_local, n_node, cap, cw).astype(half)
                for i in plane:
                    remote(
                        answer.at[mb, c, i], parts.at[sec, mb, c, local],
                        part_send.at[mb], part_recv.at[sec, mb, c], section=1, local=i,
                    ).start()

        @pl.when(sec == 0)
        def _():
            for c in range(chunks):
                remote(
                    answer.at[mb, c, local], parts.at[0, mb, c, local],
                    part_send.at[mb], part_recv.at[0, mb, c], section=1,
                ).start()

        return carry

    def collect(layer, mb, c):
        if layer == 0:
            got(parts.at[0, mb, c], part_recv.at[0, mb, c])
            rows = sum(parts[0, mb, c, i].astype(jnp.float32) for i in range(n_local))
        else:
            got(parts.at[1, mb, c, pl.ds(0, n_local - 1)], part_recv.at[1, mb, c])
            rows = answer[mb, c, local].astype(jnp.float32)
            for i in plane:
                rows = rows + parts[1, mb, c, i].astype(jnp.float32)
        summed[layer, mb, c] = rows.astype(half)
        for j in others:
            remote(
                summed.at[layer, mb, c, j], back.at[layer, mb, c, node],
                back_send.at[layer, mb], back_recv.at[layer, mb, c], node=j,
            ).start()
        back[layer, mb, c, node] = summed[layer, mb, c, node]

    def combine(layer, mb, base, where):
        for c in range(chunks):
            got(back.at[layer, mb, c, pl.ds(0, n_node - 1)], back_recv.at[layer, mb, c])
            mixed = jnp.dot(
                (first_t if layer == 0 else hits_t)[mb], flat(back[layer, mb, c]),
                preferred_element_type=jnp.float32,
            )
            cols = slice(c * cw, (c + 1) * cw)
            where[mb, :, cols] = (base[mb, :, cols].astype(jnp.float32) + mixed).astype(half)

    @pl.when(sec == 0)
    def _():
        pack(0, tok[0])
        with NS("barrier"):
            pl.semaphore_wait(barrier, 1 + n_node - 1 + 2 * (n_local - 1))

        def z_out(mb):
            for j in others:
                remote(
                    packed.at[mb, j], relay.at[mb, node], z_send.at[mb],
                    z_recv.at[0, mb, node], section=1, node=j,
                ).start()

        z_out(0)
        own_fan(0, own_recv.at[0])
        note_weights()
        for j in others:
            remote(
                meta_out.at[j], meta_z.at[node], mz_send, mz_recv.at[0, node], section=1, node=j
            ).start()
        for i in plane:
            remote(meta_out.at[node], meta_in.at[me], mo_send, mo_recv, local=i).start()
        for mb in range(1, micro):
            pack(mb, tok[mb])
            z_out(mb)
        remote(hits_t, first_t, first_send, first_recv, section=1).start()
        with NS("metawait"):
            got(meta_in.at[pl.ds(0, n_local - 1)], mo_recv)
            got(meta_in.at[pl.ds(0, (n_node - 1) * n_local)], mf_recv)
        places()
        for mb in range(1, micro):
            own_fan(mb, own_recv.at[mb])

    @pl.when(sec == 1)
    def _():
        with NS("barrier"):
            pl.semaphore_wait(barrier, 1 + 2 * (n_node - 1) + 2 * (n_local - 1))

        def hand_first(mb, nodes):
            for j in nodes:
                got(relay.at[mb, j], z_recv.at[0, mb, j])
                for i in plane + [local]:
                    remote(
                        relay.at[mb, j], arrived.at[mb, local, j],
                        fan_send.at[0, mb], fan_recv.at[mb], section=0, local=i,
                    ).start()

        note_weights()
        with NS("hand0"):
            hand_first(0, others[:-1])
        with NS("relaymeta"):
            for j in others:
                got(meta_z.at[j], mz_recv.at[0, j])
                for i in plane + [local]:
                    remote(
                        meta_z.at[j], meta_in.at[local * n_node + j], mf_send.at[0], mf_recv,
                        section=0, local=i,
                    ).start()
        with NS("hand0b"):
            hand_first(0, others[-1:])
        for j in others:
            remote(
                meta_out.at[j], meta_in.at[me], mz_send, mz_recv.at[1, node], node=j
            ).start()
        for i in plane:
            remote(meta_out.at[node], meta_in.at[me], mo_send, mo_recv, local=i).start()
        for mb in range(1, micro):
            with NS(f"hand{mb}"):
                hand_first(mb, others)
        with NS("handm"):
            for j in others:
                block = meta_in.at[local * n_node + j]
                got(block, mz_recv.at[1, j])
                for i in plane:
                    remote(block, block, mf_send.at[1], mf_recv, local=i).start()
        with NS("metawait"):
            got(meta_in.at[pl.ds(0, n_local - 1)], mo_recv)
            got(meta_in.at[pl.ds(0, (n_node - 1) * (n_local - 1))], mf_recv)
            got(first_t, first_recv)
        places()

        def dispatch(mb):
            pack(mb, held[mb])
            for j in others:
                remote(
                    packed.at[mb, j], arrived.at[mb, local, node], z_send.at[mb],
                    z_recv.at[1, mb, node], node=j,
                ).start()
            own_fan(mb, fan_recv.at[mb])
            remote(
                held.at[mb], held.at[mb], relay_send.at[mb], relay_recv.at[mb], section=0
            ).start()

        with NS("collect00"):
            for c in range(chunks):
                collect(0, 0, c)
        with NS("combine00"):
            combine(0, 0, tok, held)
        dispatch(0)
        for mb in range(1, micro):
            for c in range(chunks):
                with NS(f"collect0{mb}{c}"):
                    collect(0, mb, c)
            if mb == 1:
                with NS("second0"):
                    hand_second(0)
            with NS(f"combine0{mb}"):
                combine(0, mb, tok, held)
            dispatch(mb)

    lax.fori_loop(0, micro, expert, 0)

    @pl.when(sec == 0)
    def _():
        for mb in range(micro):
            with NS(f"relaywait{mb}"):
                got(held.at[mb], relay_recv.at[mb])
            out_ref[mb] = held[mb]
        sent(meta_out.at[pl.ds(0, n_node - 1)], mz_send)
        sent(meta_in.at[pl.ds(0, n_local - 1)], mo_send)
        sent(hits_t, first_send)
        for mb in range(micro):
            sent(packed.at[mb, pl.ds(0, n_node - 1)], z_send.at[mb])
            sent(arrived.at[mb, pl.ds(0, n_local - 1), 0], own_send.at[mb])
            sent(answer.at[mb], part_send.at[mb])

    @pl.when(sec == 1)
    def _():
        for mb in range(micro):
            with NS(f"collect1{mb}"):
                for c in range(chunks):
                    collect(1, mb, c)
        for mb in range(micro):
            with NS(f"combine1{mb}"):
                combine(1, mb, held, out_ref)
        with NS("settle"):
            sent(meta_out.at[pl.ds(0, n_node - 1)], mz_send)
            sent(meta_in.at[pl.ds(0, n_local - 1)], mo_send)
            sent(meta_in.at[pl.ds(0, (n_node - 1) * n_local)], mf_send.at[0])
            sent(meta_in.at[pl.ds(0, (n_node - 1) * (n_local - 1))], mf_send.at[1])
            for mb in range(micro):
                sent(packed.at[mb, pl.ds(0, n_node - 1)], z_send.at[mb])
                sent(arrived.at[mb, pl.ds(0, n_local - 1), 0], own_send.at[mb])
                sent(arrived.at[mb, :, pl.ds(0, n_node - 1)], fan_send.at[0, mb])
                sent(arrived.at[mb, pl.ds(0, n_local - 1), pl.ds(0, n_node - 1)], fan_send.at[1, mb])
                sent(answer.at[mb, :, pl.ds(0, n_local - 1)], part_send.at[mb])
                for layer in range(2):
                    sent(summed.at[layer, mb, :, pl.ds(0, n_node - 1)], back_send.at[layer, mb])
                sent(held.at[mb], relay_send.at[mb])


def solution(mesh):
    n_sec, n_node, n_local = mesh.shape["section"], mesh.shape["node"], mesh.shape["local"]
    n = n_node * n_local
    assert n_sec == 2

    def on_device(tokens, expert_ids, slots, gates, gain, w_gate, w_up, w_down):
        micro, toks, width = tokens.shape
        hidden = w_gate.shape[3]
        cap = 2 * toks // n_node
        limit = 4 * toks
        total = n * cap
        chunks = width // 256
        ff_chunks = hidden // 512
        cw = width // chunks
        sizes = (n_node, n_local, micro, toks, width, cap, limit, chunks, ff_chunks)
        half, full = jnp.bfloat16, jnp.float32
        vmem = pl.BlockSpec(memory_space=pltpu.VMEM)
        hbm = pl.BlockSpec(memory_space=pl.ANY)
        dma = pltpu.SemaphoreType.DMA
        mem = pltpu.VMEM
        out = pl.pallas_call(
            functools.partial(relay_kernel, sizes),
            out_shape=jax.ShapeDtypeStruct((micro, toks, width), half),
            in_specs=[hbm] * 8,
            out_specs=vmem,
            scratch_shapes=[
                mem((micro, toks, width), half),
                mem((micro, 2, toks), jnp.int32),
                mem((micro, 2, toks), jnp.int32),
                mem((micro, 2, toks), full),
                mem((1, width), full),
                mem((micro, toks, width), half),
                mem((micro, n_node, cap, width), half),
                mem((micro, n_node, cap, width), half),
                mem((micro, n_local, n_node, cap, width), half),
                mem((micro, chunks, n_local, n_node, cap, cw), half),
                mem((2, micro, chunks, n_local, n_node, cap, cw), half),
                mem((2, micro, chunks, n_node, cap, cw), half),
                mem((2, micro, chunks, n_node, cap, cw), half),
                mem((micro, n_node * cap, toks), half),
                mem((micro, toks, n_node * cap), half),
                mem((micro, toks, n_node * cap), half),
                mem((n_node, micro * n_local, LANES), full),
                mem((n_node, micro * n_local, LANES), full),
                mem((n, micro * n_local, LANES), full),
                mem((micro, limit, total), half),
                mem((micro, total, limit), half),
                mem((micro, limit, 1), full),
                mem((limit, width), half),
                mem((limit, hidden), half),
                mem((chunks, limit, cw), half),
                mem((width, hidden), half),
                mem((width, hidden), half),
                mem((hidden, width), half),
                dma((5,)), dma((3,)),
                dma(()), dma(()),
                dma(()), dma((2, n_node)), dma(()), dma(()), dma((2,)), dma(()),
                dma((micro,)), dma((2, micro, n_node)), dma((micro,)), dma((micro,)),
                dma((2, micro)), dma((micro,)),
                dma((micro,)), dma((2, micro, chunks)),
                dma((2, micro)), dma((2, micro, chunks)),
                dma((micro,)), dma((micro,)),
            ],
            compiler_params=pltpu.CompilerParams(collective_id=0, has_side_effects=True),
        )(
            tokens, *(jnp.swapaxes(a[0], 1, 2) for a in (expert_ids, slots, gates)), gain,
            w_gate[0, 0], w_up[0, 0], w_down[0, 0],
        )
        return out[None]

    placed = (
        P(None, ("node", "local"), None),
        P("section", None, ("node", "local"), None),
        P("section", None, ("node", "local"), None),
        P("section", None, ("node", "local"), None),
        P("section", None),
        P("section", ("node", "local"), None, None),
        P("section", ("node", "local"), None, None),
        P("section", ("node", "local"), None, None),
    )
    return jax.shard_map(
        on_device,
        mesh=mesh,
        in_specs=placed,
        out_specs=P("section", None, ("node", "local"), None),
        check_vma=False,
    )
```

```python
import functools

import jax
import jax.numpy as jnp
from jax import lax
from jax.experimental import pallas as pl
from jax.experimental.pallas import tpu as pltpu
from jax.sharding import PartitionSpec as P

MESH = pl.DeviceIdType.MESH
LANES = 128
NS = jax.named_scope


def relay_kernel(
    sizes,
    tok_hbm, ids_hbm, slots_hbm, gates_hbm, gain_hbm, wg_hbm, wu_hbm, wd_hbm,
    out_ref,
    tok, ids, slots, gates, gain, held, packed, relay, arrived, answer, parts, summed, back,
    hits, hits_t, first_t, meta_out, meta_z, meta_in, pick, pick_t, pick_w,
    xs, inner, lead, scaled, wg, wu, wd,
    in_sem, w_sem, first_send, first_recv, mz_send, mz_recv, mo_send, mo_recv, mf_send, mf_recv,
    z_send, z_recv, own_send, own_recv, fan_send, fan_recv, part_send, part_recv, twin_recv,
    back_send, back_recv, relay_send, relay_recv,
):
    n_node, n_local, micro, toks, width, cap, limit, chunks, ff_chunks = sizes
    n = n_node * n_local
    total = n * cap
    cw = width // chunks
    fw = inner.shape[1] // ff_chunks
    half = jnp.bfloat16
    sec = lax.axis_index("section")
    node = lax.axis_index("node")
    local = lax.axis_index("local")
    me = local * n_node + node

    def near(k):
        if n_node != 4:
            return lax.rem(node + k, n_node)
        j = jnp.int32(0)
        for z in range(n_node):
            order = sorted((p for p in range(n_node) if p != z), key=lambda p: abs(p - z))
            j = jnp.where(node == z, order[k - 1], j)
        return j

    others = [near(k) for k in range(1, n_node)]
    across = n_local - 1 - local
    plane = [lax.rem(local + i, n_local) for i in range(1, n_local)]
    if n_local == 4:
        beside = local + 1 - 2 * lax.rem(local, 2)
        plane = [across, beside, n_local - 1 - beside]

    def remote(src, dst, send, recv, **to):
        return pltpu.make_async_remote_copy(
            src, dst, send, recv, device_id=to, device_id_type=MESH
        )

    def got(ref, sem):
        remote(ref, ref, sem, sem, section=1 - sec).wait_recv()

    def sent(ref, sem):
        remote(ref, ref, sem, sem, section=1 - sec).wait_send()

    barrier = pltpu.get_barrier_semaphore()

    def greet(**to):
        pl.semaphore_signal(barrier, inc=1, device_id=to, device_id_type=MESH)

    greet(section=1 - sec)
    for j in others:
        greet(section=1 - sec, node=j)
    for i in plane:
        greet(local=i)
        greet(section=1 - sec, local=i)

    @pl.when(sec == 1)
    def _():
        for j in others:
            greet(node=j)

    loads = [
        pltpu.make_async_copy(src, dst, in_sem.at[i])
        for i, (src, dst) in enumerate(
            ((ids_hbm, ids), (slots_hbm, slots), (gates_hbm, gates), (tok_hbm, tok), (gain_hbm, gain))
        )
    ]
    for load in loads:
        load.start()
    weights_in = [
        pltpu.make_async_copy(src, dst, w_sem.at[i])
        for i, (src, dst) in enumerate(((wg_hbm, wg), (wu_hbm, wu), (wd_hbm, wd)))
    ]
    for load in loads[:3]:
        load.wait()

    slot_span = lax.broadcasted_iota(jnp.int32, (n_node * cap, toks), 0)
    for mb in range(micro):
        hit = None
        for k in range(2):
            e = ids[mb, k : k + 1, :]
            s = slots[mb, k : k + 1, :]
            pos = jnp.where(s >= 0, lax.div(e, jnp.full_like(e, n_local)) * cap + s, -1)
            this = jnp.where(pos == slot_span, 1.0, 0.0)
            hit = this if hit is None else jnp.maximum(hit, this)
        hits[mb] = hit.astype(half)
        hits_t[mb] = hit.T.astype(half)

    def note_weights():
        exp_span = lax.broadcasted_iota(jnp.int32, (n, toks), 0)
        lane_span = lax.broadcasted_iota(jnp.int32, (LANES, toks), 0)
        my_lane = lax.rem(me * cap, LANES)
        for mb in range(micro):
            named = []
            lanes = []
            for k in range(2):
                e = ids[mb, k : k + 1, :]
                s = slots[mb, k : k + 1, :]
                lane = jnp.where(s >= 0, my_lane + s, -1)
                named.append(jnp.where(e == exp_span, gates[mb, k : k + 1, :], 0.0))
                lanes.append(jnp.where(lane == lane_span, 1.0, 0.0))
            weights = lax.dot_general(
                jnp.concatenate(named, axis=1),
                jnp.concatenate(lanes, axis=1),
                (((1,), (1,)), ((), ())),
                precision=lax.Precision.HIGHEST,
                preferred_element_type=jnp.float32,
            )
            for j in range(n_node):
                meta_out[j, mb * n_local : (mb + 1) * n_local] = weights[
                    j * n_local : (j + 1) * n_local
                ]
        meta_in[me] = meta_out[node]

    note_weights()
    for load in loads[3:]:
        load.wait()
    for copy in weights_in:
        copy.start()

    def pack(mb, h):
        floats = h.astype(jnp.float32)
        mean_square = jnp.mean(floats * floats, axis=-1, keepdims=True)
        normed = (floats * lax.rsqrt(mean_square + 1e-05) * gain[...]).astype(half)
        rows = jnp.dot(hits[mb], normed, preferred_element_type=jnp.float32)
        for j in range(n_node):
            packed[mb, j] = rows[j * cap : (j + 1) * cap].astype(half)
        arrived[mb, local, node] = packed[mb, node]

    def own_fan(mb, recv):
        for i in plane:
            remote(
                packed.at[mb, node], arrived.at[mb, local, node], own_send.at[mb], recv, local=i
            ).start()

    def flat(blocks):
        if cap % 16:
            blocks = blocks.astype(jnp.float32)
        return blocks.reshape(-1, blocks.shape[-1]).astype(half)

    def places():
        upto = lax.broadcasted_iota(jnp.int32, (total, total), 0) <= lax.broadcasted_iota(
            jnp.int32, (total, total), 1
        )
        upto = jnp.where(upto, 1.0, 0.0).astype(half)
        down_span = lax.broadcasted_iota(jnp.int32, (limit, total), 0).astype(jnp.float32)
        over_span = lax.broadcasted_iota(jnp.int32, (total, limit), 1).astype(jnp.float32)
        per_group = LANES // cap
        w_rows = []
        for mb in range(micro):
            mine = pl.ds(mb * n_local + local, 1)
            w_rows.append(
                jnp.concatenate(
                    [
                        sum(meta_in[g * per_group + b, mine, :] for b in range(per_group))
                        for g in range(total // LANES)
                    ],
                    axis=1,
                )
            )
        w_all = jnp.concatenate(w_rows + [jnp.zeros((8 - micro, total), jnp.float32)], axis=0)
        chosen = jnp.where(w_all > 0.0, 1.0, 0.0)
        rank = jnp.dot(chosen.astype(half), upto, preferred_element_type=jnp.float32)
        rank = jnp.where(w_all > 0.0, rank - 1.0, -1.0)
        rank_t = rank.T
        for mb in range(micro):
            is_at = down_span == jnp.broadcast_to(rank[mb : mb + 1], (limit, total))
            pick[mb] = jnp.where(is_at, 1.0, 0.0).astype(half)
            put_at = over_span == jnp.broadcast_to(rank_t[:, mb : mb + 1], (total, limit))
            pick_t[mb] = jnp.where(put_at, 1.0, 0.0).astype(half)
            pick_w[mb] = jnp.sum(
                jnp.where(is_at, jnp.broadcast_to(w_rows[mb], (limit, total)), 0.0),
                axis=1, keepdims=True,
            )

    def hand_second(mb, nodes):
        for j in nodes:
            block = arrived.at[mb, local, j]
            got(block, z_recv.at[1, mb, j])
            for i in plane:
                remote(block, block, fan_send.at[1, mb], fan_recv.at[mb], local=i).start()

    def expert(mb, carry):
        @pl.when(sec == 0)
        def _():
            with NS("fan"):
                got(arrived.at[mb, pl.ds(0, n_local - 1), 0], own_recv.at[mb])
                got(arrived.at[mb, :, pl.ds(0, n_node - 1)], fan_recv.at[mb])

        @pl.when(sec == 1)
        def _():
            with NS("fan"):
                got(arrived.at[mb, pl.ds(0, n_local - 1)], fan_recv.at[mb])

        with NS("pick"):
            xs[...] = jnp.dot(
                pick[mb], flat(arrived[mb]), preferred_element_type=jnp.float32
            ).astype(half)

        @pl.when(mb == 0)
        def _():
            for copy in weights_in:
                copy.wait()

        def rise(between):
            with NS("up"):
                for f in range(ff_chunks):
                    cols = slice(f * fw, (f + 1) * fw)
                    x = xs[...]
                    gate = jnp.dot(x, wg[:, cols], preferred_element_type=jnp.float32)
                    up = jnp.dot(x, wu[:, cols], preferred_element_type=jnp.float32)
                    act = (jax.nn.gelu(gate, approximate=True) * up).astype(half)
                    inner[:, cols] = act
                    if f > 0:
                        prior = slice((f - 1) * fw, f * fw)
                        part = jnp.dot(
                            inner[:, prior], wd[prior, :cw], preferred_element_type=jnp.float32
                        )
                        lead[...] = part if f == 1 else lead[...] + part
                    between(f)
                last = slice((ff_chunks - 1) * fw, ff_chunks * fw)
                lead[...] += jnp.dot(
                    inner[:, last], wd[last, :cw], preferred_element_type=jnp.float32
                )

        def hand_next(f):
            done = f + 1
            if done * 3 % ff_chunks == 0:
                third = done * 3 // ff_chunks - 1
                cuts = [0, 1, 2, n_node - 1]
                hand_second(mb + 1, others[cuts[third] : cuts[third + 1]])

        busy = jnp.logical_and(sec == 1, mb + 1 < micro)

        @pl.when(busy)
        def _():
            rise(hand_next)

        @pl.when(jnp.logical_not(busy))
        def _():
            rise(lambda f: None)

        def down(c):
            acc = lead[...]
            if c > 0:
                acc = jnp.dot(
                    inner[...], wd[:, c * cw : (c + 1) * cw], preferred_element_type=jnp.float32
                )
            scaled[c] = (pick_w[mb] * acc).astype(half)

        def lay(c):
            spread = jnp.dot(pick_t[mb], scaled[c], preferred_element_type=jnp.float32)
            answer[mb, c] = spread.reshape(n_local, n_node, cap, cw).astype(half)

        def send(c):
            for i in plane:
                remote(
                    answer.at[mb, c, i], parts.at[sec, mb, c, local],
                    part_send.at[mb], part_recv.at[sec, mb, c], section=1, local=i,
                ).start()

        with NS("down"):
            down(0)
            lay(0)
            send(0)
            for c in range(1, chunks):
                down(c)
                if c > 1:
                    lay(c - 1)
            lay(chunks - 1)
            for c in range(1, chunks):
                send(c)

        @pl.when(sec == 0)
        def _():
            remote(
                answer.at[mb, :, local], parts.at[0, mb, :, local],
                part_send.at[mb], twin_recv.at[mb], section=1,
            ).start()

        return carry

    def collect(layer, mb, c):
        if layer == 0:
            got(parts.at[0, mb, c, pl.ds(0, n_local - 1)], part_recv.at[0, mb, c])
            if c == 0:
                got(parts.at[0, mb, :, local], twin_recv.at[mb])
            rows = sum(parts[0, mb, c, i].astype(jnp.float32) for i in range(n_local))
        else:
            got(parts.at[1, mb, c, pl.ds(0, n_local - 1)], part_recv.at[1, mb, c])
            rows = answer[mb, c, local].astype(jnp.float32)
            for i in plane:
                rows = rows + parts[1, mb, c, i].astype(jnp.float32)
        summed[layer, mb, c] = rows.astype(half)
        for j in others[::-1]:
            remote(
                summed.at[layer, mb, c, j], back.at[layer, mb, c, node],
                back_send.at[layer, mb], back_recv.at[layer, mb, c], node=j,
            ).start()
        back[layer, mb, c, node] = summed[layer, mb, c, node]

    def combine(layer, mb, base, where):
        for c in range(chunks):
            got(back.at[layer, mb, c, pl.ds(0, n_node - 1)], back_recv.at[layer, mb, c])
            mixed = jnp.dot(
                (first_t if layer == 0 else hits_t)[mb], flat(back[layer, mb, c]),
                preferred_element_type=jnp.float32,
            )
            cols = slice(c * cw, (c + 1) * cw)
            where[mb, :, cols] = (base[mb, :, cols].astype(jnp.float32) + mixed).astype(half)

    @pl.when(sec == 0)
    def _():
        pack(0, tok[0])
        with NS("barrier"):
            pl.semaphore_wait(barrier, 1 + n_node - 1 + 2 * (n_local - 1))

        def z_out(mb):
            for j in others:
                remote(
                    packed.at[mb, j], relay.at[mb, node], z_send.at[mb],
                    z_recv.at[0, mb, node], section=1, node=j,
                ).start()

        for j in others[::-1]:
            remote(
                meta_out.at[j], meta_z.at[node], mz_send, mz_recv.at[0, node], section=1, node=j
            ).start()
        z_out(0)
        own_fan(0, own_recv.at[0])
        for i in plane:
            remote(meta_out.at[node], meta_in.at[me], mo_send, mo_recv, local=i).start()
        for mb in range(1, micro):
            pack(mb, tok[mb])
            z_out(mb)
        remote(hits_t, first_t, first_send, first_recv, section=1).start()
        with NS("metawait"):
            got(meta_in.at[pl.ds(0, n_local - 1)], mo_recv)
            got(meta_in.at[pl.ds(0, (n_node - 1) * n_local)], mf_recv)
        places()
        for mb in range(1, micro):
            own_fan(mb, own_recv.at[mb])

    @pl.when(sec == 1)
    def _():
        with NS("barrier"):
            pl.semaphore_wait(barrier, 1 + 2 * (n_node - 1) + 2 * (n_local - 1))

        def hand_first(mb, nodes):
            for j in nodes:
                got(relay.at[mb, j], z_recv.at[0, mb, j])
                for i in plane + [local]:
                    remote(
                        relay.at[mb, j], arrived.at[mb, local, j],
                        fan_send.at[0, mb], fan_recv.at[mb], section=0, local=i,
                    ).start()

        with NS("hand0"):
            for k, j in enumerate(others):
                got(meta_z.at[j], mz_recv.at[0, j])
                for i in plane + [local]:
                    remote(
                        meta_z.at[j], meta_in.at[local * n_node + j], mf_send.at[0], mf_recv,
                        section=0, local=i,
                    ).start()
                if k == 0:
                    hand_first(0, [j])
            hand_first(0, others[1:])
        for j in others:
            remote(
                meta_out.at[j], meta_in.at[me], mz_send, mz_recv.at[1, node], node=j
            ).start()
        for i in plane:
            remote(meta_out.at[node], meta_in.at[me], mo_send, mo_recv, local=i).start()
        for mb in range(1, micro):
            with NS(f"hand{mb}"):
                hand_first(mb, others)
        with NS("handm"):
            for j in others:
                block = meta_in.at[local * n_node + j]
                got(block, mz_recv.at[1, j])
                for i in plane:
                    remote(block, block, mf_send.at[1], mf_recv, local=i).start()
        with NS("metawait"):
            got(meta_in.at[pl.ds(0, n_local - 1)], mo_recv)
            got(meta_in.at[pl.ds(0, (n_node - 1) * (n_local - 1))], mf_recv)
            got(first_t, first_recv)
        places()

        def dispatch(mb):
            pack(mb, held[mb])
            for j in others:
                remote(
                    packed.at[mb, j], arrived.at[mb, local, node], z_send.at[mb],
                    z_recv.at[1, mb, node], node=j,
                ).start()
            own_fan(mb, fan_recv.at[mb])
            remote(
                held.at[mb], held.at[mb], relay_send.at[mb], relay_recv.at[mb], section=0
            ).start()

        with NS("collect00"):
            for c in range(chunks):
                collect(0, 0, c)
        with NS("combine00"):
            combine(0, 0, tok, held)
        dispatch(0)
        for mb in range(1, micro):
            for c in range(chunks):
                with NS(f"collect0{mb}{c}"):
                    collect(0, mb, c)
            if mb == 1:
                with NS("second0"):
                    hand_second(0, others)
            with NS(f"combine0{mb}"):
                combine(0, mb, tok, held)
            dispatch(mb)

    lax.fori_loop(0, micro, expert, 0)

    @pl.when(sec == 0)
    def _():
        for mb in range(micro):
            with NS(f"relaywait{mb}"):
                got(held.at[mb], relay_recv.at[mb])
            out_ref[mb] = held[mb]
        sent(meta_out.at[pl.ds(0, n_node - 1)], mz_send)
        sent(meta_in.at[pl.ds(0, n_local - 1)], mo_send)
        sent(hits_t, first_send)
        for mb in range(micro):
            sent(packed.at[mb, pl.ds(0, n_node - 1)], z_send.at[mb])
            sent(arrived.at[mb, pl.ds(0, n_local - 1), 0], own_send.at[mb])
            sent(answer.at[mb], part_send.at[mb])

    @pl.when(sec == 1)
    def _():
        for mb in range(micro):
            with NS(f"collect1{mb}"):
                for c in range(chunks):
                    collect(1, mb, c)
        for mb in range(micro):
            with NS(f"combine1{mb}"):
                combine(1, mb, held, out_ref)
        with NS("settle"):
            sent(meta_out.at[pl.ds(0, n_node - 1)], mz_send)
            sent(meta_in.at[pl.ds(0, n_local - 1)], mo_send)
            sent(meta_in.at[pl.ds(0, (n_node - 1) * n_local)], mf_send.at[0])
            sent(meta_in.at[pl.ds(0, (n_node - 1) * (n_local - 1))], mf_send.at[1])
            for mb in range(micro):
                sent(packed.at[mb, pl.ds(0, n_node - 1)], z_send.at[mb])
                sent(arrived.at[mb, pl.ds(0, n_local - 1), 0], own_send.at[mb])
                sent(arrived.at[mb, :, pl.ds(0, n_node - 1)], fan_send.at[0, mb])
                sent(arrived.at[mb, pl.ds(0, n_local - 1), pl.ds(0, n_node - 1)], fan_send.at[1, mb])
                sent(answer.at[mb, :, pl.ds(0, n_local - 1)], part_send.at[mb])
                for layer in range(2):
                    sent(summed.at[layer, mb, :, pl.ds(0, n_node - 1)], back_send.at[layer, mb])
                sent(held.at[mb], relay_send.at[mb])


def solution(mesh):
    n_sec, n_node, n_local = mesh.shape["section"], mesh.shape["node"], mesh.shape["local"]
    n = n_node * n_local
    assert n_sec == 2

    def on_device(tokens, expert_ids, slots, gates, gain, w_gate, w_up, w_down):
        micro, toks, width = tokens.shape
        hidden = w_gate.shape[3]
        cap = 2 * toks // n_node
        limit = 4 * toks
        total = n * cap
        chunks = width // 256
        ff_chunks = hidden // 512
        cw = width // chunks
        sizes = (n_node, n_local, micro, toks, width, cap, limit, chunks, ff_chunks)
        half, full = jnp.bfloat16, jnp.float32
        vmem = pl.BlockSpec(memory_space=pltpu.VMEM)
        hbm = pl.BlockSpec(memory_space=pl.ANY)
        dma = pltpu.SemaphoreType.DMA
        mem = pltpu.VMEM
        out = pl.pallas_call(
            functools.partial(relay_kernel, sizes),
            out_shape=pltpu.VMEM((micro, toks, width), half),
            in_specs=[hbm] * 8,
            out_specs=vmem,
            scratch_shapes=[
                mem((micro, toks, width), half),
                mem((micro, 2, toks), jnp.int32),
                mem((micro, 2, toks), jnp.int32),
                mem((micro, 2, toks), full),
                mem((1, width), full),
                mem((micro, toks, width), half),
                mem((micro, n_node, cap, width), half),
                mem((micro, n_node, cap, width), half),
                mem((micro, n_local, n_node, cap, width), half),
                mem((micro, chunks, n_local, n_node, cap, cw), half),
                mem((2, micro, chunks, n_local, n_node, cap, cw), half),
                mem((2, micro, chunks, n_node, cap, cw), half),
                mem((2, micro, chunks, n_node, cap, cw), half),
                mem((micro, n_node * cap, toks), half),
                mem((micro, toks, n_node * cap), half),
                mem((micro, toks, n_node * cap), half),
                mem((n_node, micro * n_local, LANES), full),
                mem((n_node, micro * n_local, LANES), full),
                mem((n, micro * n_local, LANES), full),
                mem((micro, limit, total), half),
                mem((micro, total, limit), half),
                mem((micro, limit, 1), full),
                mem((limit, width), half),
                mem((limit, hidden), half),
                mem((limit, cw), full),
                mem((chunks, limit, cw), half),
                mem((width, hidden), half),
                mem((width, hidden), half),
                mem((hidden, width), half),
                dma((5,)), dma((3,)),
                dma(()), dma(()),
                dma(()), dma((2, n_node)), dma(()), dma(()), dma((2,)), dma(()),
                dma((micro,)), dma((2, micro, n_node)), dma((micro,)), dma((micro,)),
                dma((2, micro)), dma((micro,)),
                dma((micro,)), dma((2, micro, chunks)), dma((micro,)),
                dma((2, micro)), dma((2, micro, chunks)),
                dma((micro,)), dma((micro,)),
            ],
            compiler_params=pltpu.CompilerParams(collective_id=0, has_side_effects=True),
        )(
            tokens, *(jnp.swapaxes(a[0], 1, 2) for a in (expert_ids, slots, gates)), gain,
            w_gate[0, 0], w_up[0, 0], w_down[0, 0],
        )
        return out[None]

    placed = (
        P(None, ("node", "local"), None),
        P("section", None, ("node", "local"), None),
        P("section", None, ("node", "local"), None),
        P("section", None, ("node", "local"), None),
        P("section", None),
        P("section", ("node", "local"), None, None),
        P("section", ("node", "local"), None, None),
        P("section", ("node", "local"), None, None),
    )
    return jax.shard_map(
        on_device,
        mesh=mesh,
        in_specs=placed,
        out_specs=P("section", None, ("node", "local"), None),
        check_vma=False,
    )
```

```python
import functools

import jax
import jax.numpy as jnp
from jax import lax
from jax.experimental import pallas as pl
from jax.experimental.pallas import tpu as pltpu
from jax.sharding import PartitionSpec as P

MESH = pl.DeviceIdType.MESH
LANES = 128
NS = jax.named_scope


def relay_kernel(
    sizes,
    tok_hbm, ids_hbm, slots_hbm, gates_hbm, gain_hbm, wg_hbm, wu_hbm, wd_hbm,
    out_ref,
    tok, ids, slots, gates, gain, held, packed, relay, arrived, answer, parts, summed, back,
    hits, hits_t, first_t, meta_out, meta_z, meta_in, pick, pick_t, pick_w,
    xs, inner, lead, scaled, wg, wu, wd,
    in_sem, w_sem, first_send, first_recv, mz_send, mz_recv, mo_send, mo_recv, mf_send, mf_recv,
    z_send, z_recv, own_send, own_recv, fan_send, fan_recv, part_send, part_recv, twin_recv,
    back_send, back_recv, relay_send, relay_recv,
):
    n_node, n_local, micro, toks, width, cap, limit, chunks, ff_chunks = sizes
    n = n_node * n_local
    total = n * cap
    assert n_node * cap == LANES and n_local == 4 and limit == 2 * LANES
    cw = width // chunks
    fw = inner.shape[1] // ff_chunks
    half = jnp.bfloat16
    sec = lax.axis_index("section")
    node = lax.axis_index("node")
    local = lax.axis_index("local")
    mid = limit // 2

    def turn(i):
        return lax.rem(local + i + 1, n_local)

    mine = turn(local)

    def near(k):
        if n_node != 4:
            return lax.rem(node + k, n_node)
        j = jnp.int32(0)
        for z in range(n_node):
            order = sorted((p for p in range(n_node) if p != z), key=lambda p: abs(p - z))
            j = jnp.where(node == z, order[k - 1], j)
        return j

    others = [near(k) for k in range(1, n_node)]
    across = n_local - 1 - local
    plane = [across] + [lax.rem(across + i, n_local) for i in range(1, n_local)]
    if n_local == 4:
        beside = local + 1 - 2 * lax.rem(local, 2)
        plane = [across, beside, n_local - 1 - beside]

    def remote(src, dst, send, recv, **to):
        return pltpu.make_async_remote_copy(
            src, dst, send, recv, device_id=to, device_id_type=MESH
        )

    def got(ref, sem):
        remote(ref, ref, sem, sem, section=1 - sec).wait_recv()

    def sent(ref, sem):
        remote(ref, ref, sem, sem, section=1 - sec).wait_send()

    barrier = pltpu.get_barrier_semaphore()

    def greet(**to):
        pl.semaphore_signal(barrier, inc=1, device_id=to, device_id_type=MESH)

    greet(section=1 - sec)
    for j in others:
        greet(section=1 - sec, node=j)
    for i in plane:
        greet(local=i)
        greet(section=1 - sec, local=i)

    @pl.when(sec == 1)
    def _():
        for j in others:
            greet(node=j)

    loads = [
        pltpu.make_async_copy(src, dst, in_sem.at[i])
        for i, (src, dst) in enumerate(
            ((ids_hbm, ids), (slots_hbm, slots), (gates_hbm, gates), (tok_hbm, tok), (gain_hbm, gain))
        )
    ]
    for load in loads:
        load.start()
    weights_in = [
        pltpu.make_async_copy(src, dst, w_sem.at[i])
        for i, (src, dst) in enumerate(((wg_hbm, wg), (wu_hbm, wu), (wd_hbm, wd)))
    ]
    for load in loads[:3]:
        load.wait()

    slot_span = lax.broadcasted_iota(jnp.int32, (n_node * cap, toks), 0)
    for mb in range(micro):
        hit = None
        for k in range(2):
            e = ids[mb, k : k + 1, :]
            s = slots[mb, k : k + 1, :]
            pos = jnp.where(s >= 0, lax.div(e, jnp.full_like(e, n_local)) * cap + s, -1)
            this = jnp.where(pos == slot_span, 1.0, 0.0)
            hit = this if hit is None else jnp.maximum(hit, this)
        hits[mb] = hit.astype(half)
        hits_t[mb] = hit.T.astype(half)

    def note_weights():
        exp_span = lax.broadcasted_iota(jnp.int32, (n, toks), 0)
        lane_span = lax.broadcasted_iota(jnp.int32, (LANES, toks), 0)
        my_lane = node * cap
        for mb in range(micro):
            named = []
            lanes = []
            for k in range(2):
                e = ids[mb, k : k + 1, :]
                s = slots[mb, k : k + 1, :]
                lane = jnp.where(s >= 0, my_lane + s, -1)
                named.append(jnp.where(e == exp_span, gates[mb, k : k + 1, :], 0.0))
                lanes.append(jnp.where(lane == lane_span, 1.0, 0.0))
            weights = lax.dot_general(
                jnp.concatenate(named, axis=1),
                jnp.concatenate(lanes, axis=1),
                (((1,), (1,)), ((), ())),
                precision=lax.Precision.HIGHEST,
                preferred_element_type=jnp.float32,
            )
            for j in range(n_node):
                meta_out[j, mb * n_local : (mb + 1) * n_local] = weights[
                    j * n_local : (j + 1) * n_local
                ]
        meta_in[mine * n_node + node] = meta_out[node]

    note_weights()
    for load in loads[3:]:
        load.wait()
    for copy in weights_in:
        copy.start()

    def pack(mb, h):
        floats = h.astype(jnp.float32)
        mean_square = jnp.mean(floats * floats, axis=-1, keepdims=True)
        normed = (floats * lax.rsqrt(mean_square + 1e-05) * gain[...]).astype(half)
        rows = jnp.dot(hits[mb], normed, preferred_element_type=jnp.float32)
        for j in range(n_node):
            packed[mb, j] = rows[j * cap : (j + 1) * cap].astype(half)
        arrived[mb, mine, node] = packed[mb, node]

    def own_fan(mb, recv):
        for i in plane:
            remote(
                packed.at[mb, node], arrived.at[mb, turn(i), node], own_send.at[mb], recv, local=i
            ).start()

    def flat(blocks):
        if cap % 16:
            blocks = blocks.astype(jnp.float32)
        return blocks.reshape(-1, blocks.shape[-1]).astype(half)

    def places():
        upto = lax.broadcasted_iota(jnp.int32, (total, total), 0) <= lax.broadcasted_iota(
            jnp.int32, (total, total), 1
        )
        upto = jnp.where(upto, 1.0, 0.0).astype(half)
        down_span = lax.broadcasted_iota(jnp.int32, (limit, total), 0).astype(jnp.float32)
        over_span = lax.broadcasted_iota(jnp.int32, (total, limit), 1).astype(jnp.float32)
        per_group = LANES // cap
        w_rows = []
        for mb in range(micro):
            row = pl.ds(mb * n_local + local, 1)
            w_rows.append(
                jnp.concatenate(
                    [
                        sum(meta_in[g * per_group + b, row, :] for b in range(per_group))
                        for g in range(total // LANES)
                    ],
                    axis=1,
                )
            )
        w_all = jnp.concatenate(w_rows + [jnp.zeros((8 - micro, total), jnp.float32)], axis=0)
        chosen = jnp.where(w_all > 0.0, 1.0, 0.0)
        rank = jnp.dot(chosen.astype(half), upto, preferred_element_type=jnp.float32)
        rank = jnp.where(w_all > 0.0, rank - 1.0, -1.0)
        rank_t = rank.T
        for mb in range(micro):
            is_at = down_span == jnp.broadcast_to(rank[mb : mb + 1], (limit, total))
            pick[mb] = jnp.where(is_at, 1.0, 0.0).astype(half)
            put_at = over_span == jnp.broadcast_to(rank_t[:, mb : mb + 1], (total, limit))
            pick_t[mb] = jnp.where(put_at, 1.0, 0.0).astype(half)
            pick_w[mb] = jnp.sum(
                jnp.where(is_at, jnp.broadcast_to(w_rows[mb], (limit, total)), 0.0),
                axis=1, keepdims=True,
            )

    def hand_second(mb, nodes):
        for j in nodes:
            block = arrived.at[mb, mine, j]
            got(block, z_recv.at[1, mb, j])
            for i in plane:
                remote(
                    block, arrived.at[mb, turn(i), j], fan_send.at[1, mb], fan_recv.at[mb], local=i
                ).start()

    def collect(layer, mb, c):
        if layer == 0:
            got(parts.at[0, mb, c, pl.ds(0, n_local - 1)], part_recv.at[0, mb, c])
            if c == 0:
                got(parts.at[0, mb, :, local], twin_recv.at[mb])
            rows = sum(parts[0, mb, c, i].astype(jnp.float32) for i in range(n_local))
        else:
            got(parts.at[1, mb, c, pl.ds(0, n_local - 1)], part_recv.at[1, mb, c])
            rows = answer[mb, c, mine].astype(jnp.float32)
            for i in plane:
                rows = rows + parts[1, mb, c, i].astype(jnp.float32)
        summed[layer, mb, c] = rows.astype(half)
        for j in others[::-1]:
            remote(
                summed.at[layer, mb, c, j], back.at[layer, mb, c, node],
                back_send.at[layer, mb], back_recv.at[layer, mb, c], node=j,
            ).start()
        back[layer, mb, c, node] = summed[layer, mb, c, node]

    def expert(mb, carry):
        @pl.when(sec == 0)
        def _():
            with NS("fan"):
                got(arrived.at[mb, pl.ds(0, n_local - 1), 0], own_recv.at[mb])
                got(arrived.at[mb, :, pl.ds(0, n_node - 1)], fan_recv.at[mb])

        @pl.when(sec == 1)
        def _():
            with NS("fan"):
                got(arrived.at[mb, pl.ds(0, n_local - 1)], fan_recv.at[mb])

        @pl.when(mb == 0)
        def _():
            for copy in weights_in:
                copy.wait()

        def send(c, i):
            remote(
                answer.at[mb, c, turn(i)], parts.at[sec, mb, c, local],
                part_send.at[mb], part_recv.at[sec, mb, c], section=1, local=i,
            ).start()

        def rise(rows, leading, between):
            xs[rows] = jnp.dot(
                pick[mb, rows], flat(arrived[mb]), preferred_element_type=jnp.float32
            ).astype(half)
            for f in range(ff_chunks):
                cols = slice(f * fw, (f + 1) * fw)
                x = xs[rows]
                gate = jnp.dot(x, wg[:, cols], preferred_element_type=jnp.float32)
                up = jnp.dot(x, wu[:, cols], preferred_element_type=jnp.float32)
                inner[rows, cols] = (jax.nn.gelu(gate, approximate=True) * up).astype(half)
                if leading and f > 0:
                    prior = slice((f - 1) * fw, f * fw)
                    part = jnp.dot(
                        inner[rows, prior], wd[prior, :cw], preferred_element_type=jnp.float32
                    )
                    lead[rows] = part if f == 1 else lead[rows] + part
                between(f)
            if leading:
                last = slice((ff_chunks - 1) * fw, ff_chunks * fw)
                lead[rows] += jnp.dot(
                    inner[rows, last], wd[last, :cw], preferred_element_type=jnp.float32
                )

        def down(c, rows, acc=None):
            if acc is None:
                acc = jnp.dot(
                    inner[rows], wd[:, c * cw : (c + 1) * cw], preferred_element_type=jnp.float32
                )
            scaled[c, rows] = (pick_w[mb, rows] * acc).astype(half)

        def lay(c, first, count, depth):
            span = n_node * cap
            spread = jnp.dot(
                pick_t[mb, first * span : (first + count) * span, :depth], scaled[c, :depth],
                preferred_element_type=jnp.float32,
            )
            answer[mb, c, first : first + count] = spread.reshape(
                count, n_node, cap, cw
            ).astype(half)

        whole, top, low = slice(0, limit), slice(0, mid), slice(mid, limit)

        def finish(rows, first, targets):
            down(0, rows, lead[rows])
            lay(0, first, n_local - first, limit)
            for i in targets:
                send(0, i)
            for c in range(1, chunks):
                down(c, rows)
                if c > 1:
                    lay(c - 1, first, n_local - first, limit)
            lay(chunks - 1, first, n_local - first, limit)
            for c in range(1, chunks):
                for i in targets:
                    send(c, i)

        def hand_next(f):
            if done_at(f):
                hand_second(mb + 1, others[f * 3 // ff_chunks : f * 3 // ff_chunks + 1])
                if f == ff_chunks - 1:
                    hand_second(mb + 1, others[3:])

        def done_at(f):
            return (f + 1) * 3 % ff_chunks == 0

        def collect_prior(f):
            stops = [ff_chunks - 1, ff_chunks + 1, 2 * ff_chunks - 1]
            if micro > 1 and f in stops:
                collect(1, micro - 2, stops.index(f))

        @pl.when(jnp.logical_and(sec == 1, mb < micro - 1))
        def _():
            rise(whole, True, hand_next)
            finish(whole, 0, plane)

        @pl.when(jnp.logical_and(sec == 1, mb == micro - 1))
        def _():
            rise(top, False, collect_prior)
            down(0, top)
            for c in range(1, chunks):
                down(c, top)
                lay(c - 1, 0, 1, mid)
            lay(chunks - 1, 0, 1, mid)
            for c in range(chunks):
                send(c, plane[0])
            rise(low, True, lambda f: collect_prior(ff_chunks + f))
            finish(low, 1, plane[1:])

        @pl.when(sec == 0)
        def _():
            rise(whole, True, lambda f: None)
            finish(whole, 0, plane)

        @pl.when(sec == 0)
        def _():
            remote(
                answer.at[mb, :, mine], parts.at[0, mb, :, local],
                part_send.at[mb], twin_recv.at[mb], section=1,
            ).start()

        return carry

    def combine(layer, mb, base, where):
        for c in range(chunks):
            got(back.at[layer, mb, c, pl.ds(0, n_node - 1)], back_recv.at[layer, mb, c])
            mixed = jnp.dot(
                (first_t if layer == 0 else hits_t)[mb], flat(back[layer, mb, c]),
                preferred_element_type=jnp.float32,
            )
            cols = slice(c * cw, (c + 1) * cw)
            where[mb, :, cols] = (base[mb, :, cols].astype(jnp.float32) + mixed).astype(half)

    @pl.when(sec == 0)
    def _():
        pack(0, tok[0])
        with NS("barrier"):
            pl.semaphore_wait(barrier, 1 + n_node - 1 + 2 * (n_local - 1))

        def z_out(mb):
            for j in others:
                remote(
                    packed.at[mb, j], relay.at[mb, node], z_send.at[mb],
                    z_recv.at[0, mb, node], section=1, node=j,
                ).start()

        for j in others[::-1]:
            remote(
                meta_out.at[j], meta_z.at[node], mz_send, mz_recv.at[0, node], section=1, node=j
            ).start()
        z_out(0)
        own_fan(0, own_recv.at[0])
        for i in plane:
            remote(
                meta_out.at[node], meta_in.at[turn(i) * n_node + node], mo_send, mo_recv, local=i
            ).start()
        for mb in range(1, micro):
            pack(mb, tok[mb])
            z_out(mb)
        remote(hits_t, first_t, first_send, first_recv, section=1).start()
        with NS("metawait"):
            got(meta_in.at[pl.ds(0, n_local - 1)], mo_recv)
            got(meta_in.at[pl.ds(0, (n_node - 1) * n_local)], mf_recv)
        places()
        for mb in range(1, micro):
            own_fan(mb, own_recv.at[mb])

    @pl.when(sec == 1)
    def _():
        with NS("barrier"):
            pl.semaphore_wait(barrier, 1 + 2 * (n_node - 1) + 2 * (n_local - 1))

        def hand_first(mb, nodes):
            for j in nodes:
                got(relay.at[mb, j], z_recv.at[0, mb, j])
                for i in plane + [local]:
                    remote(
                        relay.at[mb, j], arrived.at[mb, turn(i), j],
                        fan_send.at[0, mb], fan_recv.at[mb], section=0, local=i,
                    ).start()

        with NS("hand0"):
            for k, j in enumerate(others):
                got(meta_z.at[j], mz_recv.at[0, j])
                for i in plane + [local]:
                    remote(
                        meta_z.at[j], meta_in.at[turn(i) * n_node + j], mf_send.at[0], mf_recv,
                        section=0, local=i,
                    ).start()
                if k == 0:
                    hand_first(0, [j])
            hand_first(0, others[1:])
        for j in others:
            remote(
                meta_out.at[j], meta_in.at[mine * n_node + node], mz_send,
                mz_recv.at[1, node], node=j,
            ).start()
        for i in plane:
            remote(
                meta_out.at[node], meta_in.at[turn(i) * n_node + node], mo_send, mo_recv, local=i
            ).start()
        for mb in range(1, micro):
            with NS(f"hand{mb}"):
                hand_first(mb, others)
        with NS("handm"):
            for j in others:
                block = meta_in.at[mine * n_node + j]
                got(block, mz_recv.at[1, j])
                for i in plane:
                    remote(
                        block, meta_in.at[turn(i) * n_node + j], mf_send.at[1], mf_recv, local=i
                    ).start()
        with NS("metawait"):
            got(meta_in.at[pl.ds(0, n_local - 1)], mo_recv)
            got(meta_in.at[pl.ds(0, (n_node - 1) * (n_local - 1))], mf_recv)
            got(first_t, first_recv)
        places()

        def dispatch(mb):
            pack(mb, held[mb])
            for j in others:
                remote(
                    packed.at[mb, j], arrived.at[mb, mine, node], z_send.at[mb],
                    z_recv.at[1, mb, node], node=j,
                ).start()
            own_fan(mb, fan_recv.at[mb])
            remote(
                held.at[mb], held.at[mb], relay_send.at[mb], relay_recv.at[mb], section=0
            ).start()

        with NS("collect00"):
            for c in range(chunks):
                collect(0, 0, c)
        with NS("combine00"):
            combine(0, 0, tok, held)
        dispatch(0)
        for mb in range(1, micro):
            for c in range(chunks):
                with NS(f"collect0{mb}{c}"):
                    collect(0, mb, c)
            if mb == 1:
                with NS("second0"):
                    hand_second(0, others)
            with NS(f"combine0{mb}"):
                combine(0, mb, tok, held)
            dispatch(mb)

    lax.fori_loop(0, micro, expert, 0)

    @pl.when(sec == 0)
    def _():
        for mb in range(micro):
            with NS(f"relaywait{mb}"):
                got(held.at[mb], relay_recv.at[mb])
            out_ref[mb] = held[mb]
        sent(meta_out.at[pl.ds(0, n_node - 1)], mz_send)
        sent(meta_in.at[pl.ds(0, n_local - 1)], mo_send)
        sent(hits_t, first_send)
        for mb in range(micro):
            sent(packed.at[mb, pl.ds(0, n_node - 1)], z_send.at[mb])
            sent(arrived.at[mb, pl.ds(0, n_local - 1), 0], own_send.at[mb])
            sent(answer.at[mb], part_send.at[mb])

    @pl.when(sec == 1)
    def _():
        with NS("collect11"):
            for c in range(chunks):
                collect(1, micro - 1, c)
        for mb in range(micro):
            with NS(f"combine1{mb}"):
                combine(1, mb, held, out_ref)
        with NS("settle"):
            sent(meta_out.at[pl.ds(0, n_node - 1)], mz_send)
            sent(meta_in.at[pl.ds(0, n_local - 1)], mo_send)
            sent(meta_in.at[pl.ds(0, (n_node - 1) * n_local)], mf_send.at[0])
            sent(meta_in.at[pl.ds(0, (n_node - 1) * (n_local - 1))], mf_send.at[1])
            for mb in range(micro):
                sent(packed.at[mb, pl.ds(0, n_node - 1)], z_send.at[mb])
                sent(arrived.at[mb, pl.ds(0, n_local - 1), 0], own_send.at[mb])
                sent(arrived.at[mb, :, pl.ds(0, n_node - 1)], fan_send.at[0, mb])
                sent(arrived.at[mb, pl.ds(0, n_local - 1), pl.ds(0, n_node - 1)], fan_send.at[1, mb])
                sent(answer.at[mb, :, pl.ds(0, n_local - 1)], part_send.at[mb])
                for layer in range(2):
                    sent(summed.at[layer, mb, :, pl.ds(0, n_node - 1)], back_send.at[layer, mb])
                sent(held.at[mb], relay_send.at[mb])


def solution(mesh):
    n_sec, n_node, n_local = mesh.shape["section"], mesh.shape["node"], mesh.shape["local"]
    n = n_node * n_local
    assert n_sec == 2

    def on_device(tokens, expert_ids, slots, gates, gain, w_gate, w_up, w_down):
        micro, toks, width = tokens.shape
        hidden = w_gate.shape[3]
        cap = 2 * toks // n_node
        limit = 4 * toks
        total = n * cap
        chunks = width // 256
        ff_chunks = hidden // 512
        cw = width // chunks
        sizes = (n_node, n_local, micro, toks, width, cap, limit, chunks, ff_chunks)
        half, full = jnp.bfloat16, jnp.float32
        vmem = pl.BlockSpec(memory_space=pltpu.VMEM)
        hbm = pl.BlockSpec(memory_space=pl.ANY)
        dma = pltpu.SemaphoreType.DMA
        mem = pltpu.VMEM
        out = pl.pallas_call(
            functools.partial(relay_kernel, sizes),
            out_shape=pltpu.VMEM((micro, toks, width), half),
            in_specs=[hbm] * 8,
            out_specs=vmem,
            scratch_shapes=[
                mem((micro, toks, width), half),
                mem((micro, 2, toks), jnp.int32),
                mem((micro, 2, toks), jnp.int32),
                mem((micro, 2, toks), full),
                mem((1, width), full),
                mem((micro, toks, width), half),
                mem((micro, n_node, cap, width), half),
                mem((micro, n_node, cap, width), half),
                mem((micro, n_local, n_node, cap, width), half),
                mem((micro, chunks, n_local, n_node, cap, cw), half),
                mem((2, micro, chunks, n_local, n_node, cap, cw), half),
                mem((2, micro, chunks, n_node, cap, cw), half),
                mem((2, micro, chunks, n_node, cap, cw), half),
                mem((micro, n_node * cap, toks), half),
                mem((micro, toks, n_node * cap), half),
                mem((micro, toks, n_node * cap), half),
                mem((n_node, micro * n_local, LANES), full),
                mem((n_node, micro * n_local, LANES), full),
                mem((n, micro * n_local, LANES), full),
                mem((micro, limit, total), half),
                mem((micro, total, limit), half),
                mem((micro, limit, 1), full),
                mem((limit, width), half),
                mem((limit, hidden), half),
                mem((limit, cw), full),
                mem((chunks, limit, cw), half),
                mem((width, hidden), half),
                mem((width, hidden), half),
                mem((hidden, width), half),
                dma((5,)), dma((3,)),
                dma(()), dma(()),
                dma(()), dma((2, n_node)), dma(()), dma(()), dma((2,)), dma(()),
                dma((micro,)), dma((2, micro, n_node)), dma((micro,)), dma((micro,)),
                dma((2, micro)), dma((micro,)),
                dma((micro,)), dma((2, micro, chunks)), dma((micro,)),
                dma((2, micro)), dma((2, micro, chunks)),
                dma((micro,)), dma((micro,)),
            ],
            compiler_params=pltpu.CompilerParams(collective_id=0, has_side_effects=True),
        )(
            tokens, *(jnp.swapaxes(a[0], 1, 2) for a in (expert_ids, slots, gates)), gain,
            w_gate[0, 0], w_up[0, 0], w_down[0, 0],
        )
        return out[None]

    placed = (
        P(None, ("node", "local"), None),
        P("section", None, ("node", "local"), None),
        P("section", None, ("node", "local"), None),
        P("section", None, ("node", "local"), None),
        P("section", None),
        P("section", ("node", "local"), None, None),
        P("section", ("node", "local"), None, None),
        P("section", ("node", "local"), None, None),
    )
    return jax.shard_map(
        on_device,
        mesh=mesh,
        in_specs=placed,
        out_specs=P("section", None, ("node", "local"), None),
        check_vma=False,
    )
```

```python
import functools

import jax
import jax.numpy as jnp
from jax import lax
from jax.experimental import pallas as pl
from jax.experimental.pallas import tpu as pltpu
from jax.sharding import PartitionSpec as P

MESH = pl.DeviceIdType.MESH
LANES = 128
NS = jax.named_scope


def relay_kernel(
    sizes,
    tok_hbm, ids_hbm, slots_hbm, gates_hbm, gain_hbm, wg_hbm, wu_hbm, wd_hbm,
    out_ref,
    tok, ids, slots, gates, gain, held, packed, relay, arrived, answer, parts, summed, back,
    hits, hits_t, first_t, meta_out, meta_z, meta_in, pick, pick_t, pick_w,
    xs, inner, lead, scaled, wg, wu, wd,
    in_sem, w_sem, first_send, first_recv, mz_send, mz_recv, hz_recv, mo_send, mo_recv, mf_send, mf_recv,
    z_send, z_recv, own_send, own_recv, fan_send, fan_recv, part_send, part_recv, twin_recv,
    back_send, back_recv, relay_send, relay_recv,
):
    n_node, n_local, micro, toks, width, cap, limit, chunks, ff_chunks = sizes
    n = n_node * n_local
    total = n * cap
    assert n_node * cap == LANES and n_local == 4 and limit == 2 * LANES
    cw = width // chunks
    fw = inner.shape[1] // ff_chunks
    half = jnp.bfloat16
    sec = lax.axis_index("section")
    node = lax.axis_index("node")
    local = lax.axis_index("local")
    mid = limit // 2

    def turn(i):
        return lax.rem(local + i + 1, n_local)

    mine = turn(local)

    def near(k):
        if n_node != 4:
            return lax.rem(node + k, n_node)
        j = jnp.int32(0)
        for z in range(n_node):
            order = sorted((p for p in range(n_node) if p != z), key=lambda p: abs(p - z))
            j = jnp.where(node == z, order[k - 1], j)
        return j

    others = [near(k) for k in range(1, n_node)]
    across = n_local - 1 - local
    plane = [across] + [lax.rem(across + i, n_local) for i in range(1, n_local)]
    if n_local == 4:
        beside = local + 1 - 2 * lax.rem(local, 2)
        plane = [across, beside, n_local - 1 - beside]

    def remote(src, dst, send, recv, **to):
        return pltpu.make_async_remote_copy(
            src, dst, send, recv, device_id=to, device_id_type=MESH
        )

    def got(ref, sem):
        remote(ref, ref, sem, sem, section=1 - sec).wait_recv()

    def sent(ref, sem):
        remote(ref, ref, sem, sem, section=1 - sec).wait_send()

    barrier = pltpu.get_barrier_semaphore()

    def greet(**to):
        pl.semaphore_signal(barrier, inc=1, device_id=to, device_id_type=MESH)

    greet(section=1 - sec)
    for j in others:
        greet(section=1 - sec, node=j)
    for i in plane:
        greet(local=i)
        greet(section=1 - sec, local=i)

    @pl.when(sec == 1)
    def _():
        for j in others:
            greet(node=j)

    loads = [
        pltpu.make_async_copy(src, dst, in_sem.at[i])
        for i, (src, dst) in enumerate(
            ((ids_hbm, ids), (slots_hbm, slots), (gates_hbm, gates), (tok_hbm, tok), (gain_hbm, gain))
        )
    ]
    for load in loads:
        load.start()
    weights_in = [
        pltpu.make_async_copy(src, dst, w_sem.at[i])
        for i, (src, dst) in enumerate(((wg_hbm, wg), (wu_hbm, wu), (wd_hbm, wd)))
    ]
    for load in loads[:3]:
        load.wait()

    slot_span = lax.broadcasted_iota(jnp.int32, (n_node * cap, toks), 0)
    for mb in range(micro):
        hit = None
        for k in range(2):
            e = ids[mb, k : k + 1, :]
            s = slots[mb, k : k + 1, :]
            pos = jnp.where(s >= 0, lax.div(e, jnp.full_like(e, n_local)) * cap + s, -1)
            this = jnp.where(pos == slot_span, 1.0, 0.0)
            hit = this if hit is None else jnp.maximum(hit, this)
        hits[mb] = hit.astype(half)
        hits_t[mb] = hit.T.astype(half)

    def note_weights():
        exp_span = lax.broadcasted_iota(jnp.int32, (n, toks), 0)
        lane_span = lax.broadcasted_iota(jnp.int32, (LANES, toks), 0)
        my_lane = node * cap
        for mb in range(micro):
            named = []
            lanes = []
            for k in range(2):
                e = ids[mb, k : k + 1, :]
                s = slots[mb, k : k + 1, :]
                lane = jnp.where(s >= 0, my_lane + s, -1)
                named.append(jnp.where(e == exp_span, gates[mb, k : k + 1, :], 0.0))
                lanes.append(jnp.where(lane == lane_span, 1.0, 0.0))
            weights = lax.dot_general(
                jnp.concatenate(named, axis=1),
                jnp.concatenate(lanes, axis=1),
                (((1,), (1,)), ((), ())),
                precision=lax.Precision.HIGHEST,
                preferred_element_type=jnp.float32,
            )
            for j in range(n_node):
                meta_out[j, mb * n_local : (mb + 1) * n_local] = weights[
                    j * n_local : (j + 1) * n_local
                ]
        meta_in[mine * n_node + node] = meta_out[node]

    note_weights()
    for load in loads[3:]:
        load.wait()
    for copy in weights_in:
        copy.start()

    def pack(mb, h):
        floats = h.astype(jnp.float32)
        mean_square = jnp.mean(floats * floats, axis=-1, keepdims=True)
        normed = (floats * lax.rsqrt(mean_square + 1e-05) * gain[...]).astype(half)
        rows = jnp.dot(hits[mb], normed, preferred_element_type=jnp.float32)
        for j in range(n_node):
            packed[mb, j] = rows[j * cap : (j + 1) * cap].astype(half)
        arrived[mb, mine, node] = packed[mb, node]

    def own_fan(mb, recv):
        for i in plane:
            remote(
                packed.at[mb, node], arrived.at[mb, turn(i), node], own_send, recv, local=i
            ).start()

    def flat(blocks):
        if cap % 16:
            blocks = blocks.astype(jnp.float32)
        return blocks.reshape(-1, blocks.shape[-1]).astype(half)

    def places():
        upto = lax.broadcasted_iota(jnp.int32, (total, total), 0) <= lax.broadcasted_iota(
            jnp.int32, (total, total), 1
        )
        upto = jnp.where(upto, 1.0, 0.0).astype(half)
        down_span = lax.broadcasted_iota(jnp.int32, (limit, total), 0).astype(jnp.float32)
        over_span = lax.broadcasted_iota(jnp.int32, (total, limit), 1).astype(jnp.float32)
        per_group = LANES // cap
        w_rows = []
        for mb in range(micro):
            row = pl.ds(mb * n_local + local, 1)
            w_rows.append(
                jnp.concatenate(
                    [
                        sum(meta_in[g * per_group + b, row, :] for b in range(per_group))
                        for g in range(total // LANES)
                    ],
                    axis=1,
                )
            )
        w_all = jnp.concatenate(w_rows + [jnp.zeros((8 - micro, total), jnp.float32)], axis=0)
        chosen = jnp.where(w_all > 0.0, 1.0, 0.0)
        rank = jnp.dot(chosen.astype(half), upto, preferred_element_type=jnp.float32)
        rank = jnp.where(w_all > 0.0, rank - 1.0, -1.0)
        rank_t = rank.T
        for mb in range(micro):
            is_at = down_span == jnp.broadcast_to(rank[mb : mb + 1], (limit, total))
            pick[mb] = jnp.where(is_at, 1.0, 0.0).astype(half)
            put_at = over_span == jnp.broadcast_to(rank_t[:, mb : mb + 1], (total, limit))
            pick_t[mb] = jnp.where(put_at, 1.0, 0.0).astype(half)
            pick_w[mb] = jnp.sum(
                jnp.where(is_at, jnp.broadcast_to(w_rows[mb], (limit, total)), 0.0),
                axis=1, keepdims=True,
            )

    def hand_second(mb, nodes):
        for j in nodes:
            block = arrived.at[mb, mine, j]
            got(block, z_recv.at[mb, j])
            for i in plane:
                remote(
                    block, arrived.at[mb, turn(i), j], fan_send.at[1], fan_recv.at[mb], local=i
                ).start()

    def collect(layer, mb, c):
        if layer == 0:
            got(parts.at[0, mb, c, pl.ds(0, n_local - 1)], part_recv.at[mb, c])
            if c == 0:
                got(parts.at[0, mb, :, local], twin_recv.at[mb])
            rows = sum(parts[0, mb, c, i].astype(jnp.float32) for i in range(n_local))
        else:
            got(parts.at[1, mb, c, pl.ds(0, n_local - 1)], part_recv.at[mb, c])
            rows = answer[mb, c, mine].astype(jnp.float32)
            for i in plane:
                rows = rows + parts[1, mb, c, i].astype(jnp.float32)
        summed[layer, mb, c] = rows.astype(half)
        for j in others[::-1]:
            remote(
                summed.at[layer, mb, c, j], back.at[layer, mb, c, node],
                back_send, back_recv.at[mb, c], node=j,
            ).start()
        back[layer, mb, c, node] = summed[layer, mb, c, node]

    def expert(mb, carry):
        @pl.when(sec == 0)
        def _():
            with NS("fan"):
                got(arrived.at[mb, pl.ds(0, n_local - 1), 0], own_recv.at[mb])
                got(arrived.at[mb, :, pl.ds(0, n_node - 1)], fan_recv.at[mb])

        @pl.when(sec == 1)
        def _():
            with NS("fan"):
                got(arrived.at[mb, pl.ds(0, n_local - 1)], fan_recv.at[mb])

        @pl.when(mb == 0)
        def _():
            for copy in weights_in:
                copy.wait()

        def send(c, i):
            remote(
                answer.at[mb, c, turn(i)], parts.at[sec, mb, c, local],
                part_send, part_recv.at[mb, c], section=1, local=i,
            ).start()

        def rise(rows, leading, between):
            xs[rows] = jnp.dot(
                pick[mb, rows], flat(arrived[mb]), preferred_element_type=jnp.float32
            ).astype(half)
            for f in range(ff_chunks):
                cols = slice(f * fw, (f + 1) * fw)
                x = xs[rows]
                gate = jnp.dot(x, wg[:, cols], preferred_element_type=jnp.float32)
                up = jnp.dot(x, wu[:, cols], preferred_element_type=jnp.float32)
                inner[rows, cols] = (jax.nn.gelu(gate, approximate=True) * up).astype(half)
                if leading and f > 0:
                    prior = slice((f - 1) * fw, f * fw)
                    part = jnp.dot(
                        inner[rows, prior], wd[prior, :cw], preferred_element_type=jnp.float32
                    )
                    lead[rows] = part if f == 1 else lead[rows] + part
                between(f)
            if leading:
                last = slice((ff_chunks - 1) * fw, ff_chunks * fw)
                lead[rows] += jnp.dot(
                    inner[rows, last], wd[last, :cw], preferred_element_type=jnp.float32
                )

        def down(c, rows, acc=None):
            if acc is None:
                acc = jnp.dot(
                    inner[rows], wd[:, c * cw : (c + 1) * cw], preferred_element_type=jnp.float32
                )
            scaled[c, rows] = (pick_w[mb, rows] * acc).astype(half)

        def lay(c, first, count, depth):
            span = n_node * cap
            spread = jnp.dot(
                pick_t[mb, first * span : (first + count) * span, :depth], scaled[c, :depth],
                preferred_element_type=jnp.float32,
            )
            answer[mb, c, first : first + count] = spread.reshape(
                count, n_node, cap, cw
            ).astype(half)

        whole, top, low = slice(0, limit), slice(0, mid), slice(mid, limit)

        def finish(rows, first, targets):
            down(0, rows, lead[rows])
            lay(0, first, n_local - first, limit)
            for i in targets:
                send(0, i)
            for c in range(1, chunks):
                down(c, rows)
                if c > 1:
                    lay(c - 1, first, n_local - first, limit)
            lay(chunks - 1, first, n_local - first, limit)
            for c in range(1, chunks):
                for i in targets:
                    send(c, i)

        def hand_next(f):
            if done_at(f):
                hand_second(mb + 1, others[f * 3 // ff_chunks : f * 3 // ff_chunks + 1])
                if f == ff_chunks - 1:
                    hand_second(mb + 1, others[3:])

        def done_at(f):
            return (f + 1) * 3 % ff_chunks == 0

        def collect_prior(f):
            if micro > 1 and f == 2 * ff_chunks - 1:
                for c in range(chunks):
                    collect(1, micro - 2, c)

        @pl.when(jnp.logical_and(sec == 1, mb < micro - 1))
        def _():
            rise(whole, True, hand_next)
            finish(whole, 0, plane)

        @pl.when(jnp.logical_and(sec == 1, mb == micro - 1))
        def _():
            rise(top, False, collect_prior)
            down(0, top)
            for c in range(1, chunks):
                down(c, top)
                lay(c - 1, 0, 1, mid)
            lay(chunks - 1, 0, 1, mid)
            for c in range(chunks):
                send(c, plane[0])
            rise(low, True, lambda f: collect_prior(ff_chunks + f))
            finish(low, 1, plane[1:])

        @pl.when(sec == 0)
        def _():
            rise(whole, True, lambda f: None)
            finish(whole, 0, plane)

        @pl.when(sec == 0)
        def _():
            remote(
                answer.at[mb, :, mine], parts.at[0, mb, :, local],
                part_send, twin_recv.at[mb], section=1,
            ).start()

        return carry

    def combine(layer, mb, base, where):
        for c in range(chunks):
            got(back.at[layer, mb, c, pl.ds(0, n_node - 1)], back_recv.at[mb, c])
            mixed = jnp.dot(
                (first_t if layer == 0 else hits_t)[mb], flat(back[layer, mb, c]),
                preferred_element_type=jnp.float32,
            )
            cols = slice(c * cw, (c + 1) * cw)
            where[mb, :, cols] = (base[mb, :, cols].astype(jnp.float32) + mixed).astype(half)

    @pl.when(sec == 0)
    def _():
        pack(0, tok[0])
        with NS("barrier"):
            pl.semaphore_wait(barrier, 1 + n_node - 1 + 2 * (n_local - 1))

        def z_out(mb):
            for j in others:
                remote(
                    packed.at[mb, j], relay.at[mb, node], z_send,
                    z_recv.at[mb, node], section=1, node=j,
                ).start()

        for j in others[::-1]:
            remote(
                meta_out.at[j], meta_z.at[node], mz_send, mz_recv.at[node], section=1, node=j
            ).start()
        z_out(0)
        own_fan(0, own_recv.at[0])
        for i in plane:
            remote(
                meta_out.at[node], meta_in.at[turn(i) * n_node + node], mo_send, mo_recv, local=i
            ).start()
        for mb in range(1, micro):
            pack(mb, tok[mb])
            z_out(mb)
        remote(hits_t, first_t, first_send, first_recv, section=1).start()
        with NS("metawait"):
            got(meta_in.at[pl.ds(0, n_local - 1)], mo_recv)
            got(meta_in.at[pl.ds(0, (n_node - 1) * n_local)], mf_recv)
        places()
        for mb in range(1, micro):
            own_fan(mb, own_recv.at[mb])

    @pl.when(sec == 1)
    def _():
        with NS("barrier"):
            pl.semaphore_wait(barrier, 1 + 2 * (n_node - 1) + 2 * (n_local - 1))

        def hand_first(mb, nodes):
            for j in nodes:
                got(relay.at[mb, j], z_recv.at[mb, j])
                for i in plane + [local]:
                    remote(
                        relay.at[mb, j], arrived.at[mb, turn(i), j],
                        fan_send.at[0], fan_recv.at[mb], section=0, local=i,
                    ).start()

        with NS("hand0"):
            for k, j in enumerate(others):
                got(meta_z.at[j], mz_recv.at[j])
                for i in plane + [local]:
                    remote(
                        meta_z.at[j], meta_in.at[turn(i) * n_node + j], mf_send.at[0], mf_recv,
                        section=0, local=i,
                    ).start()
                if k == 0:
                    hand_first(0, [j])
            hand_first(0, others[1:])
        for j in others:
            remote(
                meta_out.at[j], meta_in.at[mine * n_node + node], mz_send,
                hz_recv, node=j,
            ).start()
        for i in plane:
            remote(
                meta_out.at[node], meta_in.at[turn(i) * n_node + node], mo_send, mo_recv, local=i
            ).start()
        for mb in range(1, micro):
            with NS(f"hand{mb}"):
                hand_first(mb, others)
        with NS("handm"):
            got(meta_in.at[pl.ds(0, n_node - 1)], hz_recv)
            for j in others:
                block = meta_in.at[mine * n_node + j]
                for i in plane:
                    remote(
                        block, meta_in.at[turn(i) * n_node + j], mf_send.at[1], mf_recv, local=i
                    ).start()
        with NS("metawait"):
            got(meta_in.at[pl.ds(0, n_local - 1)], mo_recv)
            got(meta_in.at[pl.ds(0, (n_node - 1) * (n_local - 1))], mf_recv)
            got(first_t, first_recv)
        places()

        def dispatch(mb):
            pack(mb, held[mb])
            for j in others:
                remote(
                    packed.at[mb, j], arrived.at[mb, mine, node], z_send,
                    z_recv.at[mb, node], node=j,
                ).start()
            own_fan(mb, fan_recv.at[mb])
            remote(
                held.at[mb], held.at[mb], relay_send, relay_recv.at[mb], section=0
            ).start()

        with NS("collect00"):
            for c in range(chunks):
                collect(0, 0, c)
        with NS("combine00"):
            combine(0, 0, tok, held)
        dispatch(0)
        for mb in range(1, micro):
            for c in range(chunks):
                with NS(f"collect0{mb}{c}"):
                    collect(0, mb, c)
            if mb == 1:
                with NS("second0"):
                    hand_second(0, others)
            with NS(f"combine0{mb}"):
                combine(0, mb, tok, held)
            dispatch(mb)

    lax.fori_loop(0, micro, expert, 0)

    @pl.when(sec == 0)
    def _():
        for mb in range(micro):
            with NS(f"relaywait{mb}"):
                got(held.at[mb], relay_recv.at[mb])
            out_ref[mb] = held[mb]
        sent(meta_out.at[pl.ds(0, n_node - 1)], mz_send)
        sent(meta_in.at[pl.ds(0, n_local - 1)], mo_send)
        sent(hits_t, first_send)
        sent(packed.at[:, pl.ds(0, n_node - 1)], z_send)
        sent(arrived.at[:, pl.ds(0, n_local - 1), 0], own_send)
        sent(answer, part_send)

    @pl.when(sec == 1)
    def _():
        with NS("collect11"):
            for c in range(chunks):
                collect(1, micro - 1, c)
        for mb in range(micro):
            with NS(f"combine1{mb}"):
                combine(1, mb, held, out_ref)
        with NS("settle"):
            sent(meta_out.at[pl.ds(0, n_node - 1)], mz_send)
            sent(meta_in.at[pl.ds(0, n_local - 1)], mo_send)
            sent(meta_in.at[pl.ds(0, (n_node - 1) * n_local)], mf_send.at[0])
            sent(meta_in.at[pl.ds(0, (n_node - 1) * (n_local - 1))], mf_send.at[1])
            sent(packed.at[:, pl.ds(0, n_node - 1)], z_send)
            sent(arrived.at[:, pl.ds(0, n_local - 1), 0], own_send)
            sent(arrived.at[:, :, pl.ds(0, n_node - 1)], fan_send.at[0])
            sent(arrived.at[:, pl.ds(0, n_local - 1), pl.ds(0, n_node - 1)], fan_send.at[1])
            sent(answer.at[:, :, pl.ds(0, n_local - 1)], part_send)
            sent(summed.at[:, :, :, pl.ds(0, n_node - 1)], back_send)
            sent(held, relay_send)


def solution(mesh):
    n_sec, n_node, n_local = mesh.shape["section"], mesh.shape["node"], mesh.shape["local"]
    n = n_node * n_local
    assert n_sec == 2

    def on_device(tokens, expert_ids, slots, gates, gain, w_gate, w_up, w_down):
        micro, toks, width = tokens.shape
        hidden = w_gate.shape[3]
        cap = 2 * toks // n_node
        limit = 4 * toks
        total = n * cap
        chunks = width // 256
        ff_chunks = hidden // 512
        cw = width // chunks
        sizes = (n_node, n_local, micro, toks, width, cap, limit, chunks, ff_chunks)
        half, full = jnp.bfloat16, jnp.float32
        vmem = pl.BlockSpec(memory_space=pltpu.VMEM)
        hbm = pl.BlockSpec(memory_space=pl.ANY)
        dma = pltpu.SemaphoreType.DMA
        mem = pltpu.VMEM
        out = pl.pallas_call(
            functools.partial(relay_kernel, sizes),
            out_shape=pltpu.VMEM((micro, toks, width), half),
            in_specs=[hbm] * 8,
            out_specs=vmem,
            scratch_shapes=[
                mem((micro, toks, width), half),
                mem((micro, 2, toks), jnp.int32),
                mem((micro, 2, toks), jnp.int32),
                mem((micro, 2, toks), full),
                mem((1, width), full),
                mem((micro, toks, width), half),
                mem((micro, n_node, cap, width), half),
                mem((micro, n_node, cap, width), half),
                mem((micro, n_local, n_node, cap, width), half),
                mem((micro, chunks, n_local, n_node, cap, cw), half),
                mem((2, micro, chunks, n_local, n_node, cap, cw), half),
                mem((2, micro, chunks, n_node, cap, cw), half),
                mem((2, micro, chunks, n_node, cap, cw), half),
                mem((micro, n_node * cap, toks), half),
                mem((micro, toks, n_node * cap), half),
                mem((micro, toks, n_node * cap), half),
                mem((n_node, micro * n_local, LANES), full),
                mem((n_node, micro * n_local, LANES), full),
                mem((n, micro * n_local, LANES), full),
                mem((micro, limit, total), half),
                mem((micro, total, limit), half),
                mem((micro, limit, 1), full),
                mem((limit, width), half),
                mem((limit, hidden), half),
                mem((limit, cw), full),
                mem((chunks, limit, cw), half),
                mem((width, hidden), half),
                mem((width, hidden), half),
                mem((hidden, width), half),
                dma((5,)), dma((3,)),
                dma(()), dma(()),
                dma(()), dma((n_node,)), dma(()), dma(()), dma(()), dma((2,)), dma(()),
                dma(()), dma((micro, n_node)), dma(()), dma((micro,)),
                dma((2,)), dma((micro,)),
                dma(()), dma((micro, chunks)), dma((micro,)),
                dma(()), dma((micro, chunks)),
                dma(()), dma((micro,)),
            ],
            compiler_params=pltpu.CompilerParams(collective_id=0, has_side_effects=True),
        )(
            tokens, *(jnp.swapaxes(a[0], 1, 2) for a in (expert_ids, slots, gates)), gain,
            w_gate[0, 0], w_up[0, 0], w_down[0, 0],
        )
        return out[None]

    placed = (
        P(None, ("node", "local"), None),
        P("section", None, ("node", "local"), None),
        P("section", None, ("node", "local"), None),
        P("section", None, ("node", "local"), None),
        P("section", None),
        P("section", ("node", "local"), None, None),
        P("section", ("node", "local"), None, None),
        P("section", ("node", "local"), None, None),
    )
    return jax.shard_map(
        on_device,
        mesh=mesh,
        in_specs=placed,
        out_specs=P("section", None, ("node", "local"), None),
        check_vma=False,
    )
```

```python
import functools

import jax
import jax.numpy as jnp
from jax import lax
from jax.experimental import pallas as pl
from jax.experimental.pallas import tpu as pltpu
from jax.sharding import PartitionSpec as P

MESH = pl.DeviceIdType.MESH
LANES = 128
NS = jax.named_scope


def relay_kernel(
    sizes,
    tok_hbm, ids_hbm, slots_hbm, gates_hbm, gain_hbm, wg_hbm, wu_hbm, wd_hbm,
    out_ref,
    tok, ids, slots, gates, gain, held, packed, relay, arrived, answer, parts, summed, back,
    hits, hits_t, first_t, meta_out, meta_z, meta_in, pick, pick_t, pick_w,
    xs, inner, lead, scaled, wg, wu, wd,
    in_sem, w_sem, first_send, first_recv, mz_send, mz_recv, hz_recv, mo_send, mo_recv, mf_send, mf_recv,
    z_send, z_recv, own_send, own_recv, fan_send, fan_recv, part_send, part_recv, twin_recv,
    back_send, back_recv, relay_send, relay_recv,
):
    n_node, n_local, micro, toks, width, cap, limit, chunks, ff_chunks = sizes
    n = n_node * n_local
    total = n * cap
    assert n_node * cap == LANES and n_local == 4 and limit == 2 * LANES
    cw = width // chunks
    fw = inner.shape[1] // ff_chunks
    half = jnp.bfloat16
    sec = lax.axis_index("section")
    node = lax.axis_index("node")
    local = lax.axis_index("local")
    mid = limit // 2

    def turn(i):
        return lax.rem(local + i + 1, n_local)

    mine = turn(local)

    def near(k):
        if n_node != 4:
            return lax.rem(node + k, n_node)
        j = jnp.int32(0)
        for z in range(n_node):
            order = sorted((p for p in range(n_node) if p != z), key=lambda p: abs(p - z))
            j = jnp.where(node == z, order[k - 1], j)
        return j

    others = [near(k) for k in range(1, n_node)]
    across = n_local - 1 - local
    plane = [across] + [lax.rem(across + i, n_local) for i in range(1, n_local)]
    if n_local == 4:
        beside = local + 1 - 2 * lax.rem(local, 2)
        plane = [across, beside, n_local - 1 - beside]

    def remote(src, dst, send, recv, **to):
        return pltpu.make_async_remote_copy(
            src, dst, send, recv, device_id=to, device_id_type=MESH
        )

    def got(ref, sem):
        remote(ref, ref, sem, sem, section=1 - sec).wait_recv()

    def sent(ref, sem):
        remote(ref, ref, sem, sem, section=1 - sec).wait_send()

    barrier = pltpu.get_barrier_semaphore()

    def greet(**to):
        pl.semaphore_signal(barrier, inc=1, device_id=to, device_id_type=MESH)

    greet(section=1 - sec)
    for j in others:
        greet(section=1 - sec, node=j)
    for i in plane:
        greet(local=i)
        greet(section=1 - sec, local=i)

    @pl.when(sec == 1)
    def _():
        for j in others:
            greet(node=j)

    loads = [
        pltpu.make_async_copy(src, dst, in_sem.at[i])
        for i, (src, dst) in enumerate(
            ((ids_hbm, ids), (slots_hbm, slots), (gates_hbm, gates), (tok_hbm, tok), (gain_hbm, gain))
        )
    ]
    for load in loads:
        load.start()
    weights_in = [
        pltpu.make_async_copy(src, dst, w_sem.at[i])
        for i, (src, dst) in enumerate(((wg_hbm, wg), (wu_hbm, wu), (wd_hbm, wd)))
    ]
    for load in loads[:3]:
        load.wait()

    slot_span = lax.broadcasted_iota(jnp.int32, (n_node * cap, toks), 0)
    for mb in range(micro):
        hit = None
        for k in range(2):
            e = ids[mb, k : k + 1, :]
            s = slots[mb, k : k + 1, :]
            pos = jnp.where(s >= 0, lax.div(e, jnp.full_like(e, n_local)) * cap + s, -1)
            this = jnp.where(pos == slot_span, 1.0, 0.0)
            hit = this if hit is None else jnp.maximum(hit, this)
        hits[mb] = hit.astype(half)
        hits_t[mb] = hit.T.astype(half)

    def note_weights():
        exp_span = lax.broadcasted_iota(jnp.int32, (n, toks), 0)
        lane_span = lax.broadcasted_iota(jnp.int32, (LANES, toks), 0)
        my_lane = node * cap
        for mb in range(micro):
            named = []
            lanes = []
            for k in range(2):
                e = ids[mb, k : k + 1, :]
                s = slots[mb, k : k + 1, :]
                lane = jnp.where(s >= 0, my_lane + s, -1)
                named.append(jnp.where(e == exp_span, gates[mb, k : k + 1, :], 0.0))
                lanes.append(jnp.where(lane == lane_span, 1.0, 0.0))
            weights = lax.dot_general(
                jnp.concatenate(named, axis=1),
                jnp.concatenate(lanes, axis=1),
                (((1,), (1,)), ((), ())),
                precision=lax.Precision.HIGHEST,
                preferred_element_type=jnp.float32,
            )
            for j in range(n_node):
                meta_out[j, mb * n_local : (mb + 1) * n_local] = weights[
                    j * n_local : (j + 1) * n_local
                ]
        meta_in[mine * n_node + node] = meta_out[node]

    note_weights()
    for load in loads[3:]:
        load.wait()
    for copy in weights_in:
        copy.start()

    def pack(mb, h):
        floats = h.astype(jnp.float32)
        mean_square = jnp.mean(floats * floats, axis=-1, keepdims=True)
        normed = (floats * lax.rsqrt(mean_square + 1e-05) * gain[...]).astype(half)
        rows = jnp.dot(hits[mb], normed, preferred_element_type=jnp.float32)
        for j in range(n_node):
            packed[mb, j] = rows[j * cap : (j + 1) * cap].astype(half)
        arrived[mb, mine, node] = packed[mb, node]

    def own_fan(mb, recv):
        for i in plane:
            remote(
                packed.at[mb, node], arrived.at[mb, turn(i), node], own_send, recv, local=i
            ).start()

    def flat(blocks):
        if cap % 16:
            blocks = blocks.astype(jnp.float32)
        return blocks.reshape(-1, blocks.shape[-1]).astype(half)

    def places():
        upto = lax.broadcasted_iota(jnp.int32, (total, total), 0) <= lax.broadcasted_iota(
            jnp.int32, (total, total), 1
        )
        upto = jnp.where(upto, 1.0, 0.0).astype(half)
        down_span = lax.broadcasted_iota(jnp.int32, (limit, total), 0).astype(jnp.float32)
        over_span = lax.broadcasted_iota(jnp.int32, (total, limit), 1).astype(jnp.float32)
        per_group = LANES // cap
        w_rows = []
        for mb in range(micro):
            row = pl.ds(mb * n_local + local, 1)
            w_rows.append(
                jnp.concatenate(
                    [
                        sum(meta_in[g * per_group + b, row, :] for b in range(per_group))
                        for g in range(total // LANES)
                    ],
                    axis=1,
                )
            )
        w_all = jnp.concatenate(w_rows + [jnp.zeros((8 - micro, total), jnp.float32)], axis=0)
        chosen = jnp.where(w_all > 0.0, 1.0, 0.0)
        rank = jnp.dot(chosen.astype(half), upto, preferred_element_type=jnp.float32)
        rank = jnp.where(w_all > 0.0, rank - 1.0, -1.0)
        rank_t = rank.T
        for mb in range(micro):
            is_at = down_span == jnp.broadcast_to(rank[mb : mb + 1], (limit, total))
            pick[mb] = jnp.where(is_at, 1.0, 0.0).astype(half)
            put_at = over_span == jnp.broadcast_to(rank_t[:, mb : mb + 1], (total, limit))
            pick_t[mb] = jnp.where(put_at, 1.0, 0.0).astype(half)
            pick_w[mb] = jnp.sum(
                jnp.where(is_at, jnp.broadcast_to(w_rows[mb], (limit, total)), 0.0),
                axis=1, keepdims=True,
            )

    def hand_second(mb, nodes):
        for j in nodes:
            block = arrived.at[mb, mine, j]
            got(block, z_recv.at[mb, j])
            for i in plane:
                remote(
                    block, arrived.at[mb, turn(i), j], fan_send.at[1], fan_recv.at[mb], local=i
                ).start()

    def collect(layer, mb, c):
        if layer == 0:
            got(parts.at[0, mb, c, pl.ds(0, n_local - 1)], part_recv.at[mb, c])
            if c == 0:
                got(parts.at[0, mb, :, local], twin_recv.at[mb])
            rows = sum(parts[0, mb, c, i].astype(jnp.float32) for i in range(n_local))
        else:
            got(parts.at[1, mb, c, pl.ds(0, n_local - 1)], part_recv.at[mb, c])
            rows = answer[mb, c, mine].astype(jnp.float32)
            for i in plane:
                rows = rows + parts[1, mb, c, i].astype(jnp.float32)
        summed[layer, mb, c] = rows.astype(half)
        for j in others[::-1]:
            remote(
                summed.at[layer, mb, c, j], back.at[layer, mb, c, node],
                back_send, back_recv.at[mb, c], node=j,
            ).start()
        back[layer, mb, c, node] = summed[layer, mb, c, node]

    def expert(mb, carry):
        @pl.when(sec == 0)
        def _():
            with NS("fan"):
                got(arrived.at[mb, pl.ds(0, n_local - 1), 0], own_recv.at[mb])
                got(arrived.at[mb, :, pl.ds(0, n_node - 1)], fan_recv.at[mb])

        @pl.when(sec == 1)
        def _():
            with NS("fan"):
                got(arrived.at[mb, pl.ds(0, n_local - 1)], fan_recv.at[mb])

        @pl.when(mb == 0)
        def _():
            for copy in weights_in:
                copy.wait()

        def send(c, i):
            remote(
                answer.at[mb, c, turn(i)], parts.at[sec, mb, c, local],
                part_send, part_recv.at[mb, c], section=1, local=i,
            ).start()

        def rise(rows, leading, between):
            xs[rows] = jnp.dot(
                pick[mb, rows], flat(arrived[mb]), preferred_element_type=jnp.float32
            ).astype(half)
            for f in range(ff_chunks):
                cols = slice(f * fw, (f + 1) * fw)
                x = xs[rows]
                gate = jnp.dot(x, wg[:, cols], preferred_element_type=jnp.float32)
                up = jnp.dot(x, wu[:, cols], preferred_element_type=jnp.float32)
                inner[rows, cols] = (jax.nn.gelu(gate, approximate=True) * up).astype(half)
                if leading and f > 0:
                    prior = slice((f - 1) * fw, f * fw)
                    part = jnp.dot(
                        inner[rows, prior], wd[prior, :cw], preferred_element_type=jnp.float32
                    )
                    lead[rows] = part if f == 1 else lead[rows] + part
                between(f)
            if leading:
                last = slice((ff_chunks - 1) * fw, ff_chunks * fw)
                lead[rows] += jnp.dot(
                    inner[rows, last], wd[last, :cw], preferred_element_type=jnp.float32
                )

        def down(c, rows, acc=None):
            if acc is None:
                acc = jnp.dot(
                    inner[rows], wd[:, c * cw : (c + 1) * cw], preferred_element_type=jnp.float32
                )
            scaled[c, rows] = (pick_w[mb, rows] * acc).astype(half)

        def lay(c, first, count, depth):
            span = n_node * cap
            spread = jnp.dot(
                pick_t[mb, first * span : (first + count) * span, :depth], scaled[c, :depth],
                preferred_element_type=jnp.float32,
            )
            answer[mb, c, first : first + count] = spread.reshape(
                count, n_node, cap, cw
            ).astype(half)

        whole, top, low = slice(0, limit), slice(0, mid), slice(mid, limit)

        def finish(rows, first, targets):
            down(0, rows, lead[rows])
            lay(0, first, n_local - first, limit)
            for i in targets:
                send(0, i)
            for c in range(1, chunks):
                down(c, rows)
                if c > 1:
                    lay(c - 1, first, n_local - first, limit)
            lay(chunks - 1, first, n_local - first, limit)
            for c in range(1, chunks):
                for i in targets:
                    send(c, i)

        def hand_next(f):
            if done_at(f):
                hand_second(mb + 1, others[f * 3 // ff_chunks : f * 3 // ff_chunks + 1])
                if f == ff_chunks - 1:
                    hand_second(mb + 1, others[3:])

        def done_at(f):
            return (f + 1) * 3 % ff_chunks == 0

        @pl.when(jnp.logical_and(sec == 1, mb < micro - 1))
        def _():
            rise(whole, True, hand_next)
            finish(whole, 0, plane)

        @pl.when(jnp.logical_and(sec == 1, mb == micro - 1))
        def _():
            rise(top, False, lambda f: None)
            down(0, top)
            for c in range(1, chunks):
                down(c, top)
                lay(c - 1, 0, 1, mid)
            lay(chunks - 1, 0, 1, mid)
            for c in range(chunks):
                send(c, plane[0])
            rise(low, True, lambda f: None)
            finish(low, 1, plane[1:])

        @pl.when(sec == 0)
        def _():
            rise(whole, True, lambda f: None)
            finish(whole, 0, plane)

        @pl.when(sec == 0)
        def _():
            remote(
                answer.at[mb, :, mine], parts.at[0, mb, :, local],
                part_send, twin_recv.at[mb], section=1,
            ).start()

        return carry

    def combine(layer, mb, base, where):
        for c in range(chunks):
            got(back.at[layer, mb, c, pl.ds(0, n_node - 1)], back_recv.at[mb, c])
            mixed = jnp.dot(
                (first_t if layer == 0 else hits_t)[mb], flat(back[layer, mb, c]),
                preferred_element_type=jnp.float32,
            )
            cols = slice(c * cw, (c + 1) * cw)
            where[mb, :, cols] = (base[mb, :, cols].astype(jnp.float32) + mixed).astype(half)

    @pl.when(sec == 0)
    def _():
        pack(0, tok[0])
        with NS("barrier"):
            pl.semaphore_wait(barrier, 1 + n_node - 1 + 2 * (n_local - 1))

        def z_out(mb):
            for j in others:
                remote(
                    packed.at[mb, j], relay.at[mb, node], z_send,
                    z_recv.at[mb, node], section=1, node=j,
                ).start()

        for j in others[::-1]:
            remote(
                meta_out.at[j], meta_z.at[node], mz_send, mz_recv.at[node], section=1, node=j
            ).start()
        z_out(0)
        own_fan(0, own_recv.at[0])
        for i in plane:
            remote(
                meta_out.at[node], meta_in.at[turn(i) * n_node + node], mo_send, mo_recv, local=i
            ).start()
        for mb in range(1, micro):
            pack(mb, tok[mb])
            z_out(mb)
        remote(hits_t, first_t, first_send, first_recv, section=1).start()
        with NS("metawait"):
            got(meta_in.at[pl.ds(0, n_local - 1)], mo_recv)
            got(meta_in.at[pl.ds(0, (n_node - 1) * n_local)], mf_recv)
        places()
        for mb in range(1, micro):
            own_fan(mb, own_recv.at[mb])

    @pl.when(sec == 1)
    def _():
        with NS("barrier"):
            pl.semaphore_wait(barrier, 1 + 2 * (n_node - 1) + 2 * (n_local - 1))

        def hand_first(mb, nodes):
            for j in nodes:
                got(relay.at[mb, j], z_recv.at[mb, j])
                for i in plane + [local]:
                    remote(
                        relay.at[mb, j], arrived.at[mb, turn(i), j],
                        fan_send.at[0], fan_recv.at[mb], section=0, local=i,
                    ).start()

        with NS("hand0"):
            for k, j in enumerate(others):
                got(meta_z.at[j], mz_recv.at[j])
                for i in plane + [local]:
                    remote(
                        meta_z.at[j], meta_in.at[turn(i) * n_node + j], mf_send.at[0], mf_recv,
                        section=0, local=i,
                    ).start()
                if k == 0:
                    hand_first(0, [j])
            hand_first(0, others[1:])
        for j in others:
            remote(
                meta_out.at[j], meta_in.at[mine * n_node + node], mz_send,
                hz_recv, node=j,
            ).start()
        for i in plane:
            remote(
                meta_out.at[node], meta_in.at[turn(i) * n_node + node], mo_send, mo_recv, local=i
            ).start()
        for mb in range(1, micro):
            with NS(f"hand{mb}"):
                hand_first(mb, others)
        with NS("handm"):
            got(meta_in.at[pl.ds(0, n_node - 1)], hz_recv)
            for j in others:
                block = meta_in.at[mine * n_node + j]
                for i in plane:
                    remote(
                        block, meta_in.at[turn(i) * n_node + j], mf_send.at[1], mf_recv, local=i
                    ).start()
        with NS("metawait"):
            got(meta_in.at[pl.ds(0, n_local - 1)], mo_recv)
            got(meta_in.at[pl.ds(0, (n_node - 1) * (n_local - 1))], mf_recv)
            got(first_t, first_recv)
        places()

        def dispatch(mb):
            pack(mb, held[mb])
            for j in others:
                remote(
                    packed.at[mb, j], arrived.at[mb, mine, node], z_send,
                    z_recv.at[mb, node], node=j,
                ).start()
            own_fan(mb, fan_recv.at[mb])
            remote(
                held.at[mb], held.at[mb], relay_send, relay_recv.at[mb], section=0
            ).start()

        with NS("collect00"):
            for c in range(chunks):
                collect(0, 0, c)
        with NS("combine00"):
            combine(0, 0, tok, held)
        dispatch(0)
        for mb in range(1, micro):
            for c in range(chunks):
                with NS(f"collect0{mb}{c}"):
                    collect(0, mb, c)
            if mb == 1:
                with NS("second0"):
                    hand_second(0, others)
            with NS(f"combine0{mb}"):
                combine(0, mb, tok, held)
            dispatch(mb)

    lax.fori_loop(0, micro, expert, 0)

    @pl.when(sec == 0)
    def _():
        for mb in range(micro):
            with NS(f"relaywait{mb}"):
                got(held.at[mb], relay_recv.at[mb])
            out_ref[mb] = held[mb]
        sent(meta_out.at[pl.ds(0, n_node - 1)], mz_send)
        sent(meta_in.at[pl.ds(0, n_local - 1)], mo_send)
        sent(hits_t, first_send)
        sent(packed.at[:, pl.ds(0, n_node - 1)], z_send)
        sent(arrived.at[:, pl.ds(0, n_local - 1), 0], own_send)
        sent(answer, part_send)

    @pl.when(sec == 1)
    def _():
        with NS("collect11"):
            for mb in range(micro):
                for c in range(chunks):
                    collect(1, mb, c)
        for mb in range(micro):
            with NS(f"combine1{mb}"):
                combine(1, mb, held, out_ref)
        with NS("settle"):
            sent(meta_out.at[pl.ds(0, n_node - 1)], mz_send)
            sent(meta_in.at[pl.ds(0, n_local - 1)], mo_send)
            sent(meta_in.at[pl.ds(0, (n_node - 1) * n_local)], mf_send.at[0])
            sent(meta_in.at[pl.ds(0, (n_node - 1) * (n_local - 1))], mf_send.at[1])
            sent(packed.at[:, pl.ds(0, n_node - 1)], z_send)
            sent(arrived.at[:, pl.ds(0, n_local - 1), 0], own_send)
            sent(arrived.at[:, :, pl.ds(0, n_node - 1)], fan_send.at[0])
            sent(arrived.at[:, pl.ds(0, n_local - 1), pl.ds(0, n_node - 1)], fan_send.at[1])
            sent(answer.at[:, :, pl.ds(0, n_local - 1)], part_send)
            sent(summed.at[:, :, :, pl.ds(0, n_node - 1)], back_send)
            sent(held, relay_send)


def solution(mesh):
    n_sec, n_node, n_local = mesh.shape["section"], mesh.shape["node"], mesh.shape["local"]
    n = n_node * n_local
    assert n_sec == 2

    def on_device(tokens, expert_ids, slots, gates, gain, w_gate, w_up, w_down):
        micro, toks, width = tokens.shape
        hidden = w_gate.shape[3]
        cap = 2 * toks // n_node
        limit = 4 * toks
        total = n * cap
        chunks = width // 256
        ff_chunks = hidden // 512
        cw = width // chunks
        sizes = (n_node, n_local, micro, toks, width, cap, limit, chunks, ff_chunks)
        half, full = jnp.bfloat16, jnp.float32
        vmem = pl.BlockSpec(memory_space=pltpu.VMEM)
        hbm = pl.BlockSpec(memory_space=pl.ANY)
        dma = pltpu.SemaphoreType.DMA
        mem = pltpu.VMEM
        out = pl.pallas_call(
            functools.partial(relay_kernel, sizes),
            out_shape=pltpu.VMEM((micro, toks, width), half),
            in_specs=[hbm] * 8,
            out_specs=vmem,
            scratch_shapes=[
                mem((micro, toks, width), half),
                mem((micro, 2, toks), jnp.int32),
                mem((micro, 2, toks), jnp.int32),
                mem((micro, 2, toks), full),
                mem((1, width), full),
                mem((micro, toks, width), half),
                mem((micro, n_node, cap, width), half),
                mem((micro, n_node, cap, width), half),
                mem((micro, n_local, n_node, cap, width), half),
                mem((micro, chunks, n_local, n_node, cap, cw), half),
                mem((2, micro, chunks, n_local, n_node, cap, cw), half),
                mem((2, micro, chunks, n_node, cap, cw), half),
                mem((2, micro, chunks, n_node, cap, cw), half),
                mem((micro, n_node * cap, toks), half),
                mem((micro, toks, n_node * cap), half),
                mem((micro, toks, n_node * cap), half),
                mem((n_node, micro * n_local, LANES), full),
                mem((n_node, micro * n_local, LANES), full),
                mem((n, micro * n_local, LANES), full),
                mem((micro, limit, total), half),
                mem((micro, total, limit), half),
                mem((micro, limit, 1), full),
                mem((limit, width), half),
                mem((limit, hidden), half),
                mem((limit, cw), full),
                mem((chunks, limit, cw), half),
                mem((width, hidden), half),
                mem((width, hidden), half),
                mem((hidden, width), half),
                dma((5,)), dma((3,)),
                dma(()), dma(()),
                dma(()), dma((n_node,)), dma(()), dma(()), dma(()), dma((2,)), dma(()),
                dma(()), dma((micro, n_node)), dma(()), dma((micro,)),
                dma((2,)), dma((micro,)),
                dma(()), dma((micro, chunks)), dma((micro,)),
                dma(()), dma((micro, chunks)),
                dma(()), dma((micro,)),
            ],
            compiler_params=pltpu.CompilerParams(collective_id=0, has_side_effects=True),
        )(
            tokens, *(jnp.swapaxes(a[0], 1, 2) for a in (expert_ids, slots, gates)), gain,
            w_gate[0, 0], w_up[0, 0], w_down[0, 0],
        )
        return out[None]

    placed = (
        P(None, ("node", "local"), None),
        P("section", None, ("node", "local"), None),
        P("section", None, ("node", "local"), None),
        P("section", None, ("node", "local"), None),
        P("section", None),
        P("section", ("node", "local"), None, None),
        P("section", ("node", "local"), None, None),
        P("section", ("node", "local"), None, None),
    )
    return jax.shard_map(
        on_device,
        mesh=mesh,
        in_specs=placed,
        out_specs=P("section", None, ("node", "local"), None),
        check_vma=False,
    )
```
